8 devices in a mesh: sys: 1 (over z), row: 8 (over y, x, core).
Axes of the slice: x: 2, y: 2, z: 1, core: 2. Of those that a mesh axis runs over, the one named last changes fastest.
Arguments:
- positions: bfloat16 [8192, 128], P(('sys', 'row'))
- charges: float32 [8192], P(('sys', 'row'))
- counts: int32 [8], P(('sys', 'row'))
Outputs:
- output 1: float32 [8192, 128], P(('sys', 'row'))
- output 2: float32 [1], P('sys')
All inputs are finite; a program needn't handle non-finite values.
Results may differ from the reference program's by a relative error of at most 0.001.
Values are sent between devices in bfloat16 or wider.
A program may use at most 1 GiB of HBM per device.

```python
import jax
import jax.numpy as jnp
from jax import lax

BLOCK_ROWS = 1024
D = 128
RING_SIZE = 8
NUM_ROWS = RING_SIZE * BLOCK_ROWS
ROW_TILE = min(BLOCK_ROWS, 256)


def setup_inputs(seed: int = 0, part: int = 0) -> dict:
    part_key = jax.random.fold_in(jax.random.key(seed), part)
    sub_keys = jax.random.split(part_key, 6)
    positions = jax.random.normal(sub_keys[0], (NUM_ROWS, D), jnp.float32).astype(jnp.bfloat16)
    sign_vals = jnp.where(jax.random.bernoulli(sub_keys[1], 0.5, (NUM_ROWS,)), 1.0, -1.0)
    magnitude = jax.random.uniform(sub_keys[2], (NUM_ROWS,), jnp.float32, 0.5, 1.5)
    charges = (sign_vals * magnitude).astype(jnp.float32)
    counts = jax.random.randint(sub_keys[3], (RING_SIZE,), BLOCK_ROWS // 16, BLOCK_ROWS + 1)
    full_slot = jax.random.randint(sub_keys[4], (), 0, RING_SIZE)
    small_slot = (full_slot + jax.random.randint(sub_keys[5], (), 1, RING_SIZE)) % RING_SIZE
    counts = counts.at[full_slot].set(BLOCK_ROWS).at[small_slot].set(BLOCK_ROWS // 16)
    return {'positions': positions, 'charges': charges, 'counts': counts.astype(jnp.int32)}


def reference(positions, charges, counts):
    is_valid = jnp.arange(BLOCK_ROWS)[None, :] < counts[:, None]
    live_q = jnp.where(is_valid, charges.reshape(RING_SIZE, BLOCK_ROWS), 0.0).reshape(NUM_ROWS)
    pos_f32 = positions.astype(jnp.float32)
    sq_norm = jnp.sum(pos_f32 * pos_f32, axis=1)
    col_ids = jnp.arange(NUM_ROWS)
    neg_scale = -0.5 / D
    inv_len2 = 1.0 / D

    def tile_terms(tile_idx):
        row_start = tile_idx * ROW_TILE
        row_block = lax.dynamic_slice(positions, (row_start, 0), (ROW_TILE, D))
        row_q = lax.dynamic_slice(live_q, (row_start,), (ROW_TILE,))
        row_sq = lax.dynamic_slice(sq_norm, (row_start,), (ROW_TILE,))
        gram_mat = jnp.dot(row_block, positions.T, preferred_element_type=jnp.float32)
        dist_sq = jnp.maximum(row_sq[:, None] + sq_norm[None, :] - 2.0 * gram_mat, 0.0)
        weight = row_q[:, None] * live_q[None, :] * jnp.exp(dist_sq * neg_scale)
        row_ids = row_start + jnp.arange(ROW_TILE)
        weight = jnp.where(row_ids[:, None] == col_ids[None, :], 0.0, weight)
        pulled = jnp.dot(weight.astype(jnp.bfloat16), positions, preferred_element_type=jnp.float32)
        row_force = (jnp.sum(weight, axis=1)[:, None] * row_block.astype(jnp.float32) - pulled) * inv_len2
        return row_force, jnp.sum(weight)

    tile_forces, tile_energy = lax.map(tile_terms, jnp.arange(NUM_ROWS // ROW_TILE))
    return tile_forces.reshape(NUM_ROWS, D), (0.5 * jnp.sum(tile_energy)).reshape(1)
```

```python
import functools

import jax
import jax.numpy as jnp
from jax import lax
from jax.experimental import pallas as pl
from jax.experimental.pallas import tpu as pltpu
from jax.sharding import PartitionSpec as P

F32, BF16 = jnp.float32, jnp.bfloat16
LOG2E = 1.4426950408889634
NEG_BIG = -1e30
QUARTERS = 4
GROUPS = 6


def split3(val):
    hi = val.astype(BF16).astype(F32)
    rest = val - hi
    mid = rest.astype(BF16).astype(F32)
    low = (rest - mid).astype(BF16).astype(F32)
    return hi, mid, low


def kernel(cnt_ref, pos_hbm, q_ref, force_ref, energy_ref, xbuf, aux, xat, xai, lci, sacc, tacc, ebuf, load_sem,
           own_send, own_send_p, aux_send, aux_recv, fwd_send, ici_send, recv_p, recv_x, recv_y, prime_x, prime_y,
           e_send, e_recv):
    rows, width = pos_hbm.shape
    quarter = rows // QUARTERS
    lanes_per = quarter // 128
    me = lax.axis_index('row')
    core, ax, ay = me % 2, (me // 2) % 2, me // 4
    partner = me + 1 - 2 * core
    x_nbr = me + 2 - 4 * ax
    y_nbr = me + 4 - 8 * ay
    diag = x_nbr + 4 - 8 * ay
    off_p = 1 - 2 * core

    def rcopy(src, dst, send, recv, dev):
        return pltpu.make_async_remote_copy(src_ref=src, dst_ref=dst, send_sem=send, recv_sem=recv,
                                            device_id={'row': dev}, device_id_type=pl.DeviceIdType.MESH)

    def qref(blk, q):
        return xbuf.at[blk, pl.ds(q * quarter, quarter), :]

    load = pltpu.make_async_copy(pos_hbm, xbuf.at[me], load_sem)
    load.start()
    barrier = pltpu.get_barrier_semaphore()
    for dev in (partner, x_nbr, y_nbr):
        pl.semaphore_signal(barrier, inc=1, device_id={'row': dev}, device_id_type=pl.DeviceIdType.MESH)

    row_id = lax.broadcasted_iota(jnp.int32, (8, 128), 0) * 128 + lax.broadcasted_iota(jnp.int32, (8, 128), 1)
    live_q = jnp.where(row_id < cnt_ref[0], q_ref[...], 0.0)
    aux[me, 8:16, :] = live_q
    abs_q = jnp.abs(live_q)
    log_q = jnp.where(abs_q > 0.0, jnp.log(jnp.where(abs_q > 0.0, abs_q, 1.0)) * float(width), NEG_BIG)
    sacc[...] = jnp.zeros_like(sacc)
    tacc[...] = jnp.zeros_like(tacc)
    xat[...] = jnp.zeros_like(xat)
    load.wait()
    half_sq = []
    for grp in range(rows // 128):
        xt = jnp.transpose(xbuf[me, grp * 128:(grp + 1) * 128, :].astype(F32))
        half_sq.append(-0.5 * jnp.sum(xt * xt, axis=0, keepdims=True))
    half_sq = jnp.concatenate(half_sq, axis=0)
    aux[me, 0:8, :] = half_sq
    hi, mid, low = split3(half_sq + log_q)
    sub = lax.broadcasted_iota(jnp.int32, (128, 128), 0)
    for grp in range(rows // 128):
        sl = slice(grp * 128, (grp + 1) * 128)
        xai[sl, 0:width] = xbuf[me, sl, :]
        piece = jnp.where(sub == 0, hi[grp:grp + 1], jnp.where(sub == 1, mid[grp:grp + 1], jnp.where(
            sub == 2, low[grp:grp + 1], jnp.where(sub < 6, 1.0, 0.0))))
        xai[sl, width:2 * width] = jnp.transpose(piece).astype(BF16)
        lci[sl, :] = jnp.transpose(jnp.broadcast_to(log_q[grp:grp + 1], (128, 128)))

    pl.semaphore_wait(barrier, 3)

    sends = []
    for slot, dev in enumerate((partner, x_nbr, y_nbr)):
        cp = rcopy(aux.at[me], aux.at[me], aux_send.at[slot], aux_recv.at[slot], dev)
        cp.start()
        sends.append(cp)
    cp = rcopy(xbuf.at[me], xbuf.at[me], own_send_p, recv_p, partner)
    cp.start()
    sends.append(cp)
    for k in range(QUARTERS):
        cp = rcopy(qref(me, k), qref(me, k), own_send.at[0, k], recv_x.at[k], x_nbr)
        cp.start()
        sends.append(cp)
        qy = (k + 2) % QUARTERS
        cp = rcopy(qref(me, qy), qref(me, qy), own_send.at[1, k], recv_y.at[k], y_nbr)
        cp.start()
        sends.append(cp)

    def compute(blk_a, q_a, blk_b, q_b, own_half=None):
        chunk = 2 * quarter
        sub16 = lax.broadcasted_iota(jnp.int32, (16, quarter), 0)
        col_q = []
        xjs = []
        for side, (blk, q) in enumerate(((blk_a, q_a), (blk_b, q_b))):
            cs = slice(side * quarter, (side + 1) * quarter)
            xj = xbuf[blk, pl.ds(q * quarter, quarter), :]
            xjs.append(xj)
            xat[0:width, cs] = jnp.transpose(xj)
            srow = jnp.concatenate([aux[blk, pl.ds(q * lanes_per + t, 1), :] for t in range(lanes_per)], axis=1)
            col_q.append(jnp.concatenate(
                [aux[blk, pl.ds(8 + q * lanes_per + t, 1), :] for t in range(lanes_per)], axis=1))
            h, m, l = split3(srow)
            piece = jnp.where(sub16 < 3, 1.0, jnp.where(sub16 == 3, h, jnp.where(
                sub16 == 4, m, jnp.where(sub16 == 5, l, 0.0))))
            xat[width:width + 16, cs] = piece.astype(BF16)
        col_q = jnp.concatenate(col_q, axis=1)
        tile = 256
        for it in range(rows // tile):
            sl = slice(it * tile, (it + 1) * tile)
            gram = jnp.dot(xai[sl, :], xat[...], preferred_element_type=F32)
            cap = lci[sl, :]
            cap = jnp.concatenate([cap] * (chunk // 128), axis=1)
            weight = jnp.exp2(jnp.minimum(gram, cap) * (LOG2E / width)) * col_q
            if own_half is not None and own_half * chunk <= it * tile < (own_half + 1) * chunk:
                ri = lax.broadcasted_iota(jnp.int32, (tile, chunk), 0) + (it * tile - own_half * chunk)
                ci = lax.broadcasted_iota(jnp.int32, (tile, chunk), 1)
                weight = jnp.where(ri == ci, 0.0, weight)
            part = sacc[sl, :]
            for t in range(chunk // 128):
                part = part + weight[:, t * 128:(t + 1) * 128]
            sacc[sl, :] = part
            w_low = weight.astype(BF16)
            if VARIANT == 'a':
                tacc[sl, :] += jnp.dot(w_low[:, :quarter], xjs[0], preferred_element_type=F32) + jnp.dot(
                    w_low[:, quarter:], xjs[1], preferred_element_type=F32)
            else:
                tacc[:, sl] += lax.dot_general(xat[0:width, :], w_low, (((1,), (1,)), ((), ())),
                                               preferred_element_type=F32)

    compute(me, 0, me, 1, own_half=0)
    compute(me, 2, me, 3, own_half=1)
    rcopy(aux.at[partner], aux.at[partner], aux_send.at[0], aux_recv.at[0], partner).wait_recv()
    rcopy(xbuf.at[partner], xbuf.at[partner], own_send_p, recv_p, partner).wait_recv()

    @pl.loop(0, 2)
    def _(h):
        compute(partner, 2 * h, partner, 2 * h + 1)

    def aux_fwd(k_in, blk, slot, targets):
        rcopy(aux.at[blk], aux.at[blk], aux_send.at[0], aux_recv.at[k_in], partner).wait_recv()
        for n, (dev, k_out) in enumerate(targets):
            cp = rcopy(aux.at[blk], aux.at[blk], aux_send.at[slot + n], aux_recv.at[k_out], dev)
            cp.start()
            sends.append(cp)

    aux_fwd(1, x_nbr, 3, ((y_nbr, 3), (partner, 4)))
    aux_fwd(2, y_nbr, 5, ((partner, 5),))
    aux_fwd(3, diag, 6, ((partner, 6),))
    for k_in, blk in ((4, x_nbr), (5, y_nbr), (6, diag)):
        rcopy(aux.at[blk + off_p], aux.at[blk + off_p], aux_send.at[0], aux_recv.at[k_in], partner).wait_recv()

    @pl.loop(0, GROUPS)
    def _(k):
        far = k // QUARTERS
        blk_x = x_nbr + far * (diag - x_nbr)
        blk_y = y_nbr + far * (diag - y_nbr)
        q_x, q_y = k % QUARTERS, (k + 2) % QUARTERS
        src_x, src_y = qref(blk_x, q_x), qref(blk_y, q_y)
        rcopy(src_x, src_x, fwd_send.at[0, k], recv_x.at[k], partner).wait_recv()
        rcopy(src_x, src_x, fwd_send.at[0, k], prime_x.at[k], partner).start()

        @pl.when(k < 2)
        def _():
            rcopy(src_x, src_x, ici_send.at[0, k], recv_x.at[k + QUARTERS], y_nbr).start()

        rcopy(src_y, src_y, fwd_send.at[1, k], recv_y.at[k], partner).wait_recv()
        rcopy(src_y, src_y, fwd_send.at[1, k], prime_y.at[k], partner).start()

        @pl.when(k < 2)
        def _():
            rcopy(src_y, src_y, ici_send.at[1, k], recv_y.at[k + QUARTERS], x_nbr).start()

        @pl.loop(0, 2)
        def _(prime):
            bx, by = blk_x + prime * off_p, blk_y + prime * off_p
            px, py = qref(bx, q_x), qref(by, q_y)

            @pl.when(prime == 1)
            def _():
                rcopy(px, px, fwd_send.at[0, k], prime_x.at[k], partner).wait_recv()
                rcopy(py, py, fwd_send.at[1, k], prime_y.at[k], partner).wait_recv()

            compute(bx, q_x, by, q_y)

    total = jnp.zeros((8, 128), F32)
    live_q = aux[me, 8:16, :]
    sign = jnp.where(live_q < 0.0, -1.0, 1.0)
    for grp in range(rows // 128):
        sl = slice(grp * 128, (grp + 1) * 128)
        sign_col = jnp.transpose(jnp.broadcast_to(sign[grp:grp + 1], (128, 128)))
        row_sum = jnp.sum(sacc[sl, :], axis=1, keepdims=True)
        pulled = tacc[sl, :] if VARIANT == 'a' else jnp.transpose(tacc[:, sl])
        force_ref[sl, :] = (row_sum * xbuf[me, sl, :].astype(F32) - pulled) * (sign_col * (1.0 / width))
        signed = sacc[sl, :] * sign_col
        for t in range(16):
            total = total + signed[t * 8:(t + 1) * 8, :]
    ebuf[me] = total
    for n in range(1, 8):
        dev = (me + n) % 8
        cp = rcopy(ebuf.at[me], ebuf.at[me], e_send.at[n - 1], e_recv.at[n - 1], dev)
        cp.start()
        sends.append(cp)
    for cp in sends:
        cp.wait_send()

    @pl.loop(0, GROUPS)
    def _(k):
        for s in range(2):
            rcopy(qref(me, 0), qref(me, 0), fwd_send.at[s, k], prime_x.at[k], partner).wait_send()

    @pl.loop(0, 2)
    def _(k):
        for s in range(2):
            rcopy(qref(me, 0), qref(me, 0), ici_send.at[s, k], recv_x.at[k], partner).wait_send()

    for n in range(1, 8):
        src = (me + 8 - n) % 8
        rcopy(ebuf.at[src], ebuf.at[src], e_send.at[n - 1], e_recv.at[n - 1], src).wait_recv()
    energy_ref[0] = 0.5 * jnp.sum(jnp.sum(ebuf[...], axis=0))


VARIANT = 'b'


def solution(mesh):
    def per_device(positions, charges, counts):
        rows, width = positions.shape
        dma = pltpu.SemaphoreType.DMA
        tshape = (rows, width) if VARIANT == 'a' else (width, rows)
        forces, energy = pl.pallas_call(
            kernel,
            out_shape=(jax.ShapeDtypeStruct((rows, width), F32), jax.ShapeDtypeStruct((1,), F32)),
            in_specs=[pl.BlockSpec(memory_space=pltpu.SMEM), pl.BlockSpec(memory_space=pl.ANY),
                      pl.BlockSpec(memory_space=pltpu.VMEM)],
            out_specs=(pl.BlockSpec(memory_space=pltpu.VMEM), pl.BlockSpec(memory_space=pltpu.SMEM)),
            scratch_shapes=[
                pltpu.VMEM((8, rows, width), BF16),
                pltpu.VMEM((8, 16, 128), F32),
                pltpu.VMEM((2 * width, rows // 2), BF16),
                pltpu.VMEM((rows, 2 * width), BF16),
                pltpu.VMEM((rows, 128), F32),
                pltpu.VMEM((rows, 128), F32),
                pltpu.VMEM(tshape, F32),
                pltpu.VMEM((8, 8, 128), F32),
                dma, dma((2, QUARTERS)), dma, dma((7,)), dma((7,)), dma((2, GROUPS)), dma((2, 2)), dma,
                dma((GROUPS,)), dma((GROUPS,)), dma((GROUPS,)), dma((GROUPS,)), dma((7,)), dma((7,)),
            ],
            compiler_params=pltpu.CompilerParams(collective_id=0, has_side_effects=True),
        )(counts, positions, charges.reshape(8, 128))
        return forces, energy

    row_spec = P(('sys', 'row'), None)
    vec_spec = P(('sys', 'row'))
    return jax.shard_map(per_device, mesh=mesh, in_specs=(row_spec, vec_spec, vec_spec), out_specs=(row_spec, P('sys')),
                         check_vma=False)
```

```python
import jax
import jax.numpy as jnp
from jax import lax
from jax.experimental import pallas as pl
from jax.experimental.pallas import tpu as pltpu
from jax.sharding import PartitionSpec as P

F32, BF16 = jnp.float32, jnp.bfloat16
LOG2E = 1.4426950408889634
NEG_BIG = -1e30
QUARTERS = 4
GROUPS = 6
TILE = 256
LAG = 2
VMEM_LIMIT = 24 * 1024 * 1024


def split3(val):
    hi = val.astype(BF16).astype(F32)
    rest = val - hi
    mid = rest.astype(BF16).astype(F32)
    low = (rest - mid).astype(BF16).astype(F32)
    return hi, mid, low


def kernel(cnt_hbm, pos_hbm, q_hbm, force_ref, share_ref, xbuf, aux, xti, cap, xjt, aug, cb, sacc, tacc, qv, cnt,
           load_sem, own_send, own_send_p, aux_send, aux_recv, fwd_send, ici_send, recv_p, recv_x, recv_y, prime_x, prime_y,
           e_send, e_recv):
    rows, width = pos_hbm.shape
    quarter = rows // QUARTERS
    lanes_per = quarter // 128
    me = lax.axis_index('row')
    core, ax, ay = me % 2, (me // 2) % 2, me // 4
    off_p = 1 - 2 * core
    partner = me + off_p
    x_nbr = me + 2 - 4 * ax
    y_nbr = me + 4 - 8 * ay
    diag = x_nbr + 4 - 8 * ay

    def rcopy(src, dst, send, recv, dev):
        return pltpu.make_async_remote_copy(src_ref=src, dst_ref=dst, send_sem=send, recv_sem=recv,
                                            device_id={'row': dev}, device_id_type=pl.DeviceIdType.MESH)

    def qref(blk, q):
        return xbuf.at[blk, pl.ds(q * quarter, quarter), :]

    load = pltpu.make_async_copy(pos_hbm, xbuf.at[me], load_sem.at[0])
    load.start()
    load_q = pltpu.make_async_copy(q_hbm, qv, load_sem.at[1])
    load_q.start()
    load_c = pltpu.make_async_copy(cnt_hbm, cnt, load_sem.at[2])
    load_c.start()
    barrier = pltpu.get_barrier_semaphore()
    for dev in (partner, x_nbr, y_nbr):
        pl.semaphore_signal(barrier, inc=1, device_id={'row': dev}, device_id_type=pl.DeviceIdType.MESH)
    sends = []

    def send(cp):
        cp.start()
        sends.append(cp)

    def send_quarter(k):
        send(rcopy(qref(me, k), qref(me, k), own_send.at[0, k], recv_x.at[k], x_nbr))
        qy = (k + 2) % QUARTERS
        send(rcopy(qref(me, qy), qref(me, qy), own_send.at[1, k], recv_y.at[k], y_nbr))

    load.wait()
    with jax.named_scope('bar_wait'):
        pl.semaphore_wait(barrier, 3)
    send_quarter(0)
    load_q.wait()
    load_c.wait()

    row_id = lax.broadcasted_iota(jnp.int32, (8, 128), 0) * 128 + lax.broadcasted_iota(jnp.int32, (8, 128), 1)
    live_q = jnp.where(row_id < cnt[0], qv[...], 0.0)
    aux[me, 8:16, :] = live_q
    half_sq = []
    for grp in range(rows // 128):
        sl = slice(grp * 128, (grp + 1) * 128)
        xt = jnp.transpose(xbuf[me, sl, :])
        xti[0:width, sl] = xt
        xt = xt.astype(F32)
        half_sq.append(-0.5 * jnp.sum(xt * xt, axis=0, keepdims=True))
    half_sq = jnp.concatenate(half_sq, axis=0)
    aux[me, 0:8, :] = half_sq
    abs_q = jnp.abs(live_q)
    log_q = jnp.where(abs_q > 0.0, jnp.log(jnp.where(abs_q > 0.0, abs_q, 1.0)) * float(width), NEG_BIG)
    hi, mid, low = split3(half_sq + log_q)
    sub16 = lax.broadcasted_iota(jnp.int32, (16, 128), 0)
    for grp in range(rows // 128):
        sl = slice(grp * 128, (grp + 1) * 128)
        row = slice(grp, grp + 1)
        piece = jnp.where(sub16 < 3, 1.0, jnp.where(sub16 == 3, hi[row], jnp.where(sub16 == 4, mid[row], jnp.where(
            sub16 == 5, low[row], 0.0))))
        xti[width:width + 16, sl] = piece.astype(BF16)
        cap[0:1, sl] = log_q[row]
    xti[width + 16:2 * width, :] = jnp.zeros((width - 16, rows), BF16)
    sacc[...] = jnp.zeros_like(sacc)
    tacc[...] = jnp.zeros_like(tacc)

    for slot, dev in enumerate((x_nbr, y_nbr, partner)):
        send(rcopy(aux.at[me], aux.at[me], aux_send.at[slot], aux_recv.at[slot], dev))
    send(rcopy(xbuf.at[me], xbuf.at[me], own_send_p, recv_p, partner))
    for k in range(1, QUARTERS):
        send_quarter(k)

    def build(parts):
        sub8 = lax.broadcasted_iota(jnp.int32, (8, 128), 0)
        for n, (blk, q) in enumerate(parts):
            for t in range(lanes_per):
                sl = slice((n * lanes_per + t) * 128, (n * lanes_per + t + 1) * 128)
                grp = q * lanes_per + t
                xjt[:, sl] = jnp.transpose(xbuf[blk, pl.ds(pl.multiple_of(grp * 128, 128), 128), :])
                h, m, l = split3(aux[blk, pl.ds(grp, 1), :])
                piece = jnp.where(sub8 == 0, h, jnp.where(sub8 == 1, m, jnp.where(sub8 == 2, l, jnp.where(
                    sub8 < 6, 1.0, 0.0))))
                piece = jnp.concatenate([piece, jnp.zeros((120, 128), F32)], axis=0)
                aug[sl, :] = jnp.transpose(piece).astype(BF16)
                cb[sl, :] = jnp.transpose(jnp.broadcast_to(aux[blk, pl.ds(8 + grp, 1), :], (128, 128)))

    def compute(parts, own=False):
        build(parts)
        tiles = rows // TILE
        units = [(it, p) for it in range(tiles) for p in range(len(parts))]

        def gram(it, p):
            blk, q = parts[p]
            xj = xbuf[blk, pl.ds(pl.multiple_of(q * quarter, quarter), quarter), :]
            lhs = jnp.concatenate([xj, aug[p * quarter:(p + 1) * quarter, :]], axis=1)
            return jnp.dot(lhs, xti[:, it * TILE:(it + 1) * TILE], preferred_element_type=F32)

        grams = {}
        for unit in units[:LAG]:
            grams[unit] = gram(*unit)
        for idx, (it, p) in enumerate(units):
            sl = slice(it * TILE, (it + 1) * TILE)
            ps = slice(p * quarter, (p + 1) * quarter)
            if p == 0:
                ssum, tsum = sacc[:, sl], None
            charge = jnp.concatenate([cb[ps, :]] * (TILE // 128), axis=1)
            weight = jnp.exp2(jnp.minimum(grams.pop((it, p)), cap[0:1, sl]) * (LOG2E / width)) * charge
            if own and p == it:
                ri = lax.broadcasted_iota(jnp.int32, (TILE, TILE), 0)
                ci = lax.broadcasted_iota(jnp.int32, (TILE, TILE), 1)
                weight = jnp.where(ri == ci, 0.0, weight)
            for t in range(quarter // 8):
                ssum = ssum + weight[t * 8:(t + 1) * 8, :]
            if idx + LAG < len(units):
                grams[units[idx + LAG]] = gram(*units[idx + LAG])
            part = jnp.dot(xjt[:, ps], weight.astype(BF16), preferred_element_type=F32)
            tsum = part if tsum is None else tsum + part
            if p == len(parts) - 1:
                sacc[:, sl] = ssum
                tacc[:, sl] += tsum

    def wait_aux(k_in, blk):
        rcopy(aux.at[blk], aux.at[blk], aux_send.at[0], aux_recv.at[k_in], partner).wait_recv()

    def start_aux(slot, blk, k_out, dev):
        rcopy(aux.at[blk], aux.at[blk], aux_send.at[slot], aux_recv.at[k_out], dev).start()

    with jax.named_scope('own'):
        compute([(me, q) for q in range(QUARTERS)], own=True)
    with jax.named_scope('partner_wait'):
        wait_aux(2, partner)
        rcopy(xbuf.at[partner], xbuf.at[partner], own_send_p, recv_p, partner).wait_recv()
    with jax.named_scope('aux_wait'):
        wait_aux(0, x_nbr)
        start_aux(3, x_nbr, 3, partner)
        start_aux(4, x_nbr, 5, y_nbr)
        wait_aux(1, y_nbr)
        start_aux(5, y_nbr, 4, partner)

    def place(k):
        far = k // QUARTERS
        return (x_nbr + far * (diag - x_nbr), k % QUARTERS), (y_nbr + far * (diag - y_nbr), (k + 2) % QUARTERS)

    def pass_on(k):
        (blk_x, q_x), (blk_y, q_y) = place(k)
        src_x, src_y = qref(blk_x, q_x), qref(blk_y, q_y)
        rcopy(src_x, src_x, fwd_send.at[0, k], recv_x.at[k], partner).wait_recv()

        @pl.when(k < 2)
        def _():
            rcopy(src_x, src_x, ici_send.at[0, k], recv_x.at[k + QUARTERS], y_nbr).start()

        rcopy(src_x, src_x, fwd_send.at[0, k], prime_x.at[k], partner).start()
        rcopy(src_y, src_y, fwd_send.at[1, k], recv_y.at[k], partner).wait_recv()

        @pl.when(k < 2)
        def _():
            rcopy(src_y, src_y, ici_send.at[1, k], recv_y.at[k + QUARTERS], x_nbr).start()

        rcopy(src_y, src_y, fwd_send.at[1, k], prime_y.at[k], partner).start()

    @pl.loop(0, GROUPS + 1)
    def _(k):
        @pl.when(k < GROUPS)
        def _():
            with jax.named_scope('pass_on'):
                pass_on(k)

        @pl.when(k == 1)
        def _():
            wait_aux(3, x_nbr + off_p)
            wait_aux(4, y_nbr + off_p)
            wait_aux(5, diag)
            start_aux(6, diag, 6, partner)

        @pl.when(k == QUARTERS + 1)
        def _():
            wait_aux(6, diag + off_p)

        live = (k + GROUPS) // (GROUPS + 1)
        prev = k - live
        (blk_x, q_x), (blk_y, q_y) = place(prev)

        @pl.when(k > 0)
        def _():
            par_x, par_y = qref(blk_x + off_p, q_x), qref(blk_y + off_p, q_y)
            with jax.named_scope('wait_prime'):
                rcopy(par_x, par_x, fwd_send.at[0, prev], prime_x.at[prev], partner).wait_recv()
                rcopy(par_y, par_y, fwd_send.at[1, prev], prime_y.at[prev], partner).wait_recv()

        def pick(part, first_q):
            return partner + live * (part[0] - partner), first_q + live * (part[1] - first_q)

        with jax.named_scope('group'):
            compute([pick((blk_x, q_x), 0), pick((blk_y, q_y), 1), pick((blk_x + off_p, q_x), 2),
                     pick((blk_y + off_p, q_y), 3)])

    with jax.named_scope('share'):
        total = jnp.zeros((8, 128), F32)
        live_q = aux[me, 8:16, :]
        sign = jnp.where(live_q < 0.0, -1.0, 1.0)
        for grp in range(rows // 128):
            total = total + sacc[:, grp * 128:(grp + 1) * 128] * sign[grp:grp + 1]
        share_ref[me] = total
    for n in range(1, 8):
        dev = (me + n) % 8
        send(rcopy(share_ref.at[me], share_ref.at[me], e_send.at[n - 1], e_recv.at[n - 1], dev))
    with jax.named_scope('force'):
        for grp in range(rows // 128):
            sl = slice(grp * 128, (grp + 1) * 128)
            row_sum = jnp.sum(sacc[:, sl], axis=0, keepdims=True)
            force = (row_sum * xti[0:width, sl].astype(F32) - tacc[:, sl]) * (sign[grp:grp + 1] * (1.0 / width))
            force_ref[sl, :] = jnp.transpose(force)

    with jax.named_scope('tail'):
        for cp in sends:
            cp.wait_send()
        for slot, blk in ((3, x_nbr), (4, x_nbr), (5, y_nbr), (6, diag)):
            rcopy(aux.at[blk], aux.at[blk], aux_send.at[slot], aux_recv.at[0], partner).wait_send()

        @pl.loop(0, GROUPS)
        def _(k):
            for s in range(2):
                rcopy(qref(me, 0), qref(me, 0), fwd_send.at[s, k], prime_x.at[k], partner).wait_send()

        @pl.loop(0, 2)
        def _(k):
            for s in range(2):
                rcopy(qref(me, 0), qref(me, 0), ici_send.at[s, k], recv_x.at[k], partner).wait_send()

        for n in range(1, 8):
            src = (me + 8 - n) % 8
            rcopy(share_ref.at[src], share_ref.at[src], e_send.at[n - 1], e_recv.at[n - 1], src).wait_recv()


def finish(force_ref, share_ref, force_hbm, energy_ref, sem):
    out = pltpu.make_async_copy(force_ref, force_hbm, sem)
    out.start()
    energy_ref[0] = 0.5 * jnp.sum(jnp.sum(share_ref[...], axis=0))
    out.wait()


def solution(mesh):
    def per_device(positions, charges, counts):
        rows, width = positions.shape
        dma = pltpu.SemaphoreType.DMA
        vmem, hbm = pl.BlockSpec(memory_space=pltpu.VMEM), pl.BlockSpec(memory_space=pltpu.HBM)
        force_type = jax.ShapeDtypeStruct((rows, width), F32)
        forces, shares = pl.pallas_call(
            kernel,
            out_shape=(force_type, jax.ShapeDtypeStruct((8, 8, 128), F32)),
            in_specs=[hbm, hbm, hbm],
            out_specs=(vmem, vmem),
            scratch_shapes=[
                pltpu.VMEM((8, rows, width), BF16),
                pltpu.VMEM((8, 16, 128), F32),
                pltpu.VMEM((2 * width, rows), BF16),
                pltpu.VMEM((8, rows), F32),
                pltpu.VMEM((width, rows), BF16),
                pltpu.VMEM((rows, 128), BF16),
                pltpu.VMEM((rows, 128), F32),
                pltpu.VMEM((8, rows), F32),
                pltpu.VMEM((width, rows), F32),
                pltpu.VMEM((8, 128), F32),
                pltpu.SMEM((1,), jnp.int32),
                dma((3,)), dma((2, QUARTERS)), dma, dma((7,)), dma((7,)), dma((2, GROUPS)), dma((2, 2)), dma,
                dma((GROUPS,)), dma((GROUPS,)), dma((GROUPS,)), dma((GROUPS,)), dma((7,)), dma((7,)),
            ],
            compiler_params=pltpu.CompilerParams(collective_id=0, has_side_effects=True, vmem_limit_bytes=VMEM_LIMIT),
        )(counts, positions, charges.reshape(8, 128))
        return pl.pallas_call(
            finish,
            out_shape=(force_type, jax.ShapeDtypeStruct((1,), F32)),
            in_specs=[vmem, vmem],
            out_specs=(hbm, pl.BlockSpec(memory_space=pltpu.SMEM)),
            scratch_shapes=[dma],
            compiler_params=pltpu.CompilerParams(vmem_limit_bytes=4 * 1024 * 1024),
        )(forces, shares)

    row_spec = P(('sys', 'row'), None)
    vec_spec = P(('sys', 'row'))
    return jax.shard_map(per_device, mesh=mesh, in_specs=(row_spec, vec_spec, vec_spec), out_specs=(row_spec, P('sys')),
                         check_vma=False)
```

```python
import jax
import jax.numpy as jnp
from jax import lax
from jax.experimental import pallas as pl
from jax.experimental.pallas import tpu as pltpu
from jax.sharding import PartitionSpec as P

F32, BF16 = jnp.float32, jnp.bfloat16
LOG2E = 1.4426950408889634
NEG_BIG = -1e30
QUARTERS = 4
GROUPS = 6
TILE = 256
LAG = 4
VMEM_LIMIT = 24 * 1024 * 1024


def split3(val):
    hi = val.astype(BF16).astype(F32)
    rest = val - hi
    mid = rest.astype(BF16).astype(F32)
    low = (rest - mid).astype(BF16).astype(F32)
    return hi, mid, low


def kernel(cnt_hbm, pos_hbm, q_hbm, force_ref, share_ref, xbuf, aux, xti, cap, xjt, aug, cb, sacc, tacc, qv, cnt,
           load_sem, own_send, own_send_p, aux_send, aux_recv, fwd_send, ici_send, recv_p, recv_x, recv_y, prime_x, prime_y,
           e_send, e_recv):
    rows, width = pos_hbm.shape
    quarter = rows // QUARTERS
    lanes_per = quarter // 128
    me = lax.axis_index('row')
    core, ax, ay = me % 2, (me // 2) % 2, me // 4
    off_p = 1 - 2 * core
    partner = me + off_p
    x_nbr = me + 2 - 4 * ax
    y_nbr = me + 4 - 8 * ay
    diag = x_nbr + 4 - 8 * ay

    def rcopy(src, dst, send, recv, dev):
        return pltpu.make_async_remote_copy(src_ref=src, dst_ref=dst, send_sem=send, recv_sem=recv,
                                            device_id={'row': dev}, device_id_type=pl.DeviceIdType.MESH)

    def qref(blk, q):
        return xbuf.at[blk, pl.ds(q * quarter, quarter), :]

    load = pltpu.make_async_copy(pos_hbm, xbuf.at[me], load_sem.at[0])
    load.start()
    load_q = pltpu.make_async_copy(q_hbm, qv, load_sem.at[1])
    load_q.start()
    load_c = pltpu.make_async_copy(cnt_hbm, cnt, load_sem.at[2])
    load_c.start()
    barrier = pltpu.get_barrier_semaphore()
    for dev in (partner, x_nbr, y_nbr):
        pl.semaphore_signal(barrier, inc=1, device_id={'row': dev}, device_id_type=pl.DeviceIdType.MESH)
    sends = []

    def send(cp):
        cp.start()
        sends.append(cp)

    def send_quarter(k):
        send(rcopy(qref(me, k), qref(me, k), own_send.at[0, k], recv_x.at[k], x_nbr))
        qy = (k + 2) % QUARTERS
        send(rcopy(qref(me, qy), qref(me, qy), own_send.at[1, k], recv_y.at[k], y_nbr))

    load_q.wait()
    load_c.wait()
    row_id = lax.broadcasted_iota(jnp.int32, (8, 128), 0) * 128 + lax.broadcasted_iota(jnp.int32, (8, 128), 1)
    live_q = jnp.where(row_id < cnt[0], qv[...], 0.0)
    aux[me] = live_q
    load.wait()
    with jax.named_scope('bar_wait'):
        pl.semaphore_wait(barrier, 3)

    for slot, dev in enumerate((x_nbr, y_nbr, partner)):
        send(rcopy(aux.at[me], aux.at[me], aux_send.at[slot], aux_recv.at[slot], dev))
    send_quarter(0)
    send(rcopy(xbuf.at[me], xbuf.at[me], own_send_p, recv_p, partner))
    for k in range(1, QUARTERS):
        send_quarter(k)

    half_sq = []
    for grp in range(rows // 128):
        sl = slice(grp * 128, (grp + 1) * 128)
        xt = jnp.transpose(xbuf[me, sl, :])
        xti[0:width, sl] = xt
        xt = xt.astype(F32)
        half_sq.append(-0.5 * jnp.sum(xt * xt, axis=0, keepdims=True))
    half_sq = jnp.concatenate(half_sq, axis=0)
    abs_q = jnp.abs(live_q)
    log_q = jnp.where(abs_q > 0.0, jnp.log(jnp.where(abs_q > 0.0, abs_q, 1.0)) * float(width), NEG_BIG)
    hi, mid, low = split3(half_sq + log_q)
    sub16 = lax.broadcasted_iota(jnp.int32, (16, 128), 0)
    for grp in range(rows // 128):
        sl = slice(grp * 128, (grp + 1) * 128)
        row = slice(grp, grp + 1)
        piece = jnp.where(sub16 < 3, 1.0, jnp.where(sub16 == 3, hi[row], jnp.where(sub16 == 4, mid[row], jnp.where(
            sub16 == 5, low[row], 0.0))))
        xti[width:width + 16, sl] = piece.astype(BF16)
        cap[0:1, sl] = log_q[row]
    xti[width + 16:2 * width, :] = jnp.zeros((width - 16, rows), BF16)
    sacc[...] = jnp.zeros_like(sacc)
    tacc[...] = jnp.zeros_like(tacc)

    def build(parts):
        sub8 = lax.broadcasted_iota(jnp.int32, (8, 128), 0)
        for n, (blk, q) in enumerate(parts):
            for t in range(lanes_per):
                sl = slice((n * lanes_per + t) * 128, (n * lanes_per + t + 1) * 128)
                grp = q * lanes_per + t
                xt = jnp.transpose(xbuf[blk, pl.ds(pl.multiple_of(grp * 128, 128), 128), :])
                xjt[:, sl] = xt
                xt = xt.astype(F32)
                h, m, l = split3(-0.5 * jnp.sum(xt * xt, axis=0, keepdims=True))
                piece = jnp.where(sub8 == 0, h, jnp.where(sub8 == 1, m, jnp.where(sub8 == 2, l, jnp.where(
                    sub8 < 6, 1.0, 0.0))))
                piece = jnp.concatenate([piece, jnp.zeros((120, 128), F32)], axis=0)
                aug[sl, :] = jnp.transpose(piece).astype(BF16)
                cb[sl, :] = jnp.transpose(jnp.broadcast_to(aux[blk, pl.ds(grp, 1), :], (128, 128)))

    def compute(parts, own=False):
        build(parts)
        tiles = rows // TILE
        units = [(it, p) for it in range(tiles) for p in range(len(parts))]

        def gram(it, p):
            blk, q = parts[p]
            xj = xbuf[blk, pl.ds(pl.multiple_of(q * quarter, quarter), quarter), :]
            lhs = jnp.concatenate([xj, aug[p * quarter:(p + 1) * quarter, :]], axis=1)
            return jnp.dot(lhs, xti[:, it * TILE:(it + 1) * TILE], preferred_element_type=F32)

        grams = {}
        for unit in units[:LAG]:
            grams[unit] = gram(*unit)
        for idx, (it, p) in enumerate(units):
            sl = slice(it * TILE, (it + 1) * TILE)
            ps = slice(p * quarter, (p + 1) * quarter)
            if p == 0:
                ssum, tsum = sacc[:, sl], None
            charge = jnp.concatenate([cb[ps, :]] * (TILE // 128), axis=1)
            weight = jnp.exp2(jnp.minimum(grams.pop((it, p)), cap[0:1, sl]) * (LOG2E / width)) * charge
            if own and p == it:
                ri = lax.broadcasted_iota(jnp.int32, (TILE, TILE), 0)
                ci = lax.broadcasted_iota(jnp.int32, (TILE, TILE), 1)
                weight = jnp.where(ri == ci, 0.0, weight)
            for t in range(quarter // 8):
                ssum = ssum + weight[t * 8:(t + 1) * 8, :]
            if idx + LAG < len(units):
                grams[units[idx + LAG]] = gram(*units[idx + LAG])
            part = jnp.dot(xjt[:, ps], weight.astype(BF16), preferred_element_type=F32)
            tsum = part if tsum is None else tsum + part
            if p == len(parts) - 1:
                sacc[:, sl] = ssum
                tacc[:, sl] += tsum

    def wait_aux(k_in, blk):
        rcopy(aux.at[blk], aux.at[blk], aux_send.at[0], aux_recv.at[k_in], partner).wait_recv()

    def start_aux(slot, blk, k_out, dev):
        rcopy(aux.at[blk], aux.at[blk], aux_send.at[slot], aux_recv.at[k_out], dev).start()

    with jax.named_scope('own'):
        compute([(me, q) for q in range(QUARTERS)], own=True)
    with jax.named_scope('partner_wait'):
        wait_aux(2, partner)
        rcopy(xbuf.at[partner], xbuf.at[partner], own_send_p, recv_p, partner).wait_recv()
    with jax.named_scope('aux_wait'):
        wait_aux(0, x_nbr)
        start_aux(3, x_nbr, 3, partner)
        start_aux(4, x_nbr, 5, y_nbr)
        wait_aux(1, y_nbr)
        start_aux(5, y_nbr, 4, partner)

    def place(k):
        far = k // QUARTERS
        return (x_nbr + far * (diag - x_nbr), k % QUARTERS), (y_nbr + far * (diag - y_nbr), (k + 2) % QUARTERS)

    def pass_on(k):
        (blk_x, q_x), (blk_y, q_y) = place(k)
        src_x, src_y = qref(blk_x, q_x), qref(blk_y, q_y)
        rcopy(src_x, src_x, fwd_send.at[0, k], recv_x.at[k], partner).wait_recv()

        @pl.when(k < 2)
        def _():
            rcopy(src_x, src_x, ici_send.at[0, k], recv_x.at[k + QUARTERS], y_nbr).start()

        rcopy(src_x, src_x, fwd_send.at[0, k], prime_x.at[k], partner).start()
        rcopy(src_y, src_y, fwd_send.at[1, k], recv_y.at[k], partner).wait_recv()

        @pl.when(k < 2)
        def _():
            rcopy(src_y, src_y, ici_send.at[1, k], recv_y.at[k + QUARTERS], x_nbr).start()

        rcopy(src_y, src_y, fwd_send.at[1, k], prime_y.at[k], partner).start()

    @pl.loop(0, GROUPS + 1)
    def _(k):
        @pl.when(k < GROUPS)
        def _():
            with jax.named_scope('pass_on'):
                pass_on(k)

        @pl.when(k == 1)
        def _():
            wait_aux(3, x_nbr + off_p)
            wait_aux(4, y_nbr + off_p)
            wait_aux(5, diag)
            start_aux(6, diag, 6, partner)

        @pl.when(k == QUARTERS + 1)
        def _():
            wait_aux(6, diag + off_p)

        live = (k + GROUPS) // (GROUPS + 1)
        prev = k - live
        (blk_x, q_x), (blk_y, q_y) = place(prev)

        @pl.when(k > 0)
        def _():
            par_x, par_y = qref(blk_x + off_p, q_x), qref(blk_y + off_p, q_y)
            with jax.named_scope('wait_prime'):
                rcopy(par_x, par_x, fwd_send.at[0, prev], prime_x.at[prev], partner).wait_recv()
                rcopy(par_y, par_y, fwd_send.at[1, prev], prime_y.at[prev], partner).wait_recv()

        def pick(part, first_q):
            return partner + live * (part[0] - partner), first_q + live * (part[1] - first_q)

        with jax.named_scope('group'):
            compute([pick((blk_x, q_x), 0), pick((blk_y, q_y), 1), pick((blk_x + off_p, q_x), 2),
                     pick((blk_y + off_p, q_y), 3)])

    with jax.named_scope('share'):
        total = jnp.zeros((8, 128), F32)
        live_q = aux[me]
        sign = jnp.where(live_q < 0.0, -1.0, 1.0)
        for grp in range(rows // 128):
            total = total + sacc[:, grp * 128:(grp + 1) * 128] * sign[grp:grp + 1]
        share_ref[me] = total
    for n in range(1, 8):
        dev = (me + n) % 8
        send(rcopy(share_ref.at[me], share_ref.at[me], e_send.at[n - 1], e_recv.at[n - 1], dev))
    with jax.named_scope('force'):
        for grp in range(rows // 128):
            sl = slice(grp * 128, (grp + 1) * 128)
            row_sum = jnp.sum(sacc[:, sl], axis=0, keepdims=True)
            force = (row_sum * xti[0:width, sl].astype(F32) - tacc[:, sl]) * (sign[grp:grp + 1] * (1.0 / width))
            force_ref[sl, :] = jnp.transpose(force)

    with jax.named_scope('tail'):
        for cp in sends:
            cp.wait_send()
        for slot, blk in ((3, x_nbr), (4, x_nbr), (5, y_nbr), (6, diag)):
            rcopy(aux.at[blk], aux.at[blk], aux_send.at[slot], aux_recv.at[0], partner).wait_send()

        @pl.loop(0, GROUPS)
        def _(k):
            for s in range(2):
                rcopy(qref(me, 0), qref(me, 0), fwd_send.at[s, k], prime_x.at[k], partner).wait_send()

        @pl.loop(0, 2)
        def _(k):
            for s in range(2):
                rcopy(qref(me, 0), qref(me, 0), ici_send.at[s, k], recv_x.at[k], partner).wait_send()

        for n in range(1, 8):
            src = (me + 8 - n) % 8
            rcopy(share_ref.at[src], share_ref.at[src], e_send.at[n - 1], e_recv.at[n - 1], src).wait_recv()


def finish(force_ref, share_ref, force_hbm, energy_ref, sem):
    out = pltpu.make_async_copy(force_ref, force_hbm, sem)
    out.start()
    energy_ref[0] = 0.5 * jnp.sum(jnp.sum(share_ref[...], axis=0))
    out.wait()


def solution(mesh):
    def per_device(positions, charges, counts):
        rows, width = positions.shape
        dma = pltpu.SemaphoreType.DMA
        vmem, hbm = pl.BlockSpec(memory_space=pltpu.VMEM), pl.BlockSpec(memory_space=pltpu.HBM)
        force_type = jax.ShapeDtypeStruct((rows, width), F32)
        forces, shares = pl.pallas_call(
            kernel,
            out_shape=(force_type, jax.ShapeDtypeStruct((8, 8, 128), F32)),
            in_specs=[hbm, hbm, hbm],
            out_specs=(vmem, vmem),
            scratch_shapes=[
                pltpu.VMEM((8, rows, width), BF16),
                pltpu.VMEM((8, 8, 128), F32),
                pltpu.VMEM((2 * width, rows), BF16),
                pltpu.VMEM((8, rows), F32),
                pltpu.VMEM((width, rows), BF16),
                pltpu.VMEM((rows, 128), BF16),
                pltpu.VMEM((rows, 128), F32),
                pltpu.VMEM((8, rows), F32),
                pltpu.VMEM((width, rows), F32),
                pltpu.VMEM((8, 128), F32),
                pltpu.SMEM((1,), jnp.int32),
                dma((3,)), dma((2, QUARTERS)), dma, dma((7,)), dma((7,)), dma((2, GROUPS)), dma((2, 2)), dma,
                dma((GROUPS,)), dma((GROUPS,)), dma((GROUPS,)), dma((GROUPS,)), dma((7,)), dma((7,)),
            ],
            compiler_params=pltpu.CompilerParams(collective_id=0, has_side_effects=True, vmem_limit_bytes=VMEM_LIMIT),
        )(counts, pltpu.with_memory_space_constraint(positions, pltpu.HBM),
          pltpu.with_memory_space_constraint(charges.reshape(8, 128), pltpu.HBM))
        return pl.pallas_call(
            finish,
            out_shape=(force_type, jax.ShapeDtypeStruct((1,), F32)),
            in_specs=[vmem, vmem],
            out_specs=(hbm, pl.BlockSpec(memory_space=pltpu.SMEM)),
            scratch_shapes=[dma],
            compiler_params=pltpu.CompilerParams(vmem_limit_bytes=4 * 1024 * 1024),
        )(forces, shares)

    row_spec = P(('sys', 'row'), None)
    vec_spec = P(('sys', 'row'))
    return jax.shard_map(per_device, mesh=mesh, in_specs=(row_spec, vec_spec, vec_spec), out_specs=(row_spec, P('sys')),
                         check_vma=False)
```

```python
import jax
import jax.numpy as jnp
from jax import lax
from jax.experimental import pallas as pl
from jax.experimental.pallas import tpu as pltpu
from jax.sharding import PartitionSpec as P

F32, BF16 = jnp.float32, jnp.bfloat16
LOG2E = 1.4426950408889634
NEG_BIG = -1e30
QUARTERS = 4
GROUPS = 6
TILE = 256
LAG = 4
VMEM_LIMIT = 24 * 1024 * 1024


def split3(val):
    hi = val.astype(BF16).astype(F32)
    rest = val - hi
    mid = rest.astype(BF16).astype(F32)
    low = (rest - mid).astype(BF16).astype(F32)
    return hi, mid, low


def kernel(cnt_hbm, pos_hbm, q_hbm, force_ref, share_ref, xbuf, aux, xti, cap, xjt, aug, cb, sacc, tacc, qv, cnt,
           load_sem, row_send, aux_send, aux_recv, recv_p, recv_x, recv_y, prime, e_send, e_recv):
    rows, width = pos_hbm.shape
    quarter = rows // QUARTERS
    lanes_per = quarter // 128
    me = lax.axis_index('row')
    core, ax, ay = me % 2, (me // 2) % 2, me // 4
    off_p = 1 - 2 * core
    partner = me + off_p
    x_nbr = me + 2 - 4 * ax
    y_nbr = me + 4 - 8 * ay
    diag = x_nbr + 4 - 8 * ay

    def rcopy(src, dst, send, recv, dev):
        return pltpu.make_async_remote_copy(src_ref=src, dst_ref=dst, send_sem=send, recv_sem=recv,
                                            device_id={'row': dev}, device_id_type=pl.DeviceIdType.MESH)

    def qref(blk, q):
        return xbuf.at[blk, pl.ds(q * quarter, quarter), :]

    load = pltpu.make_async_copy(pos_hbm, xbuf.at[me], load_sem.at[0])
    load.start()
    load_q = pltpu.make_async_copy(q_hbm, qv, load_sem.at[1])
    load_q.start()
    load_c = pltpu.make_async_copy(cnt_hbm, cnt, load_sem.at[2])
    load_c.start()
    barrier = pltpu.get_barrier_semaphore()
    for dev in (partner, x_nbr, y_nbr):
        pl.semaphore_signal(barrier, inc=1, device_id={'row': dev}, device_id_type=pl.DeviceIdType.MESH)

    def send_quarter(k):
        rcopy(qref(me, k), qref(me, k), row_send, recv_x.at[k], x_nbr).start()
        qy = (k + 2) % QUARTERS
        rcopy(qref(me, qy), qref(me, qy), row_send, recv_y.at[k], y_nbr).start()

    load_q.wait()
    load_c.wait()
    row_id = lax.broadcasted_iota(jnp.int32, (8, 128), 0) * 128 + lax.broadcasted_iota(jnp.int32, (8, 128), 1)
    live_q = jnp.where(row_id < cnt[0], qv[...], 0.0)
    aux[me] = live_q
    load.wait()
    with jax.named_scope('bar_wait'):
        pl.semaphore_wait(barrier, 3)

    for slot, dev in ((0, x_nbr), (0, y_nbr), (1, partner)):
        rcopy(aux.at[me], aux.at[me], aux_send, aux_recv.at[slot], dev).start()
    send_quarter(0)
    rcopy(xbuf.at[me], xbuf.at[me], row_send, recv_p, partner).start()
    for k in range(1, QUARTERS):
        send_quarter(k)

    half_sq = []
    for grp in range(rows // 128):
        sl = slice(grp * 128, (grp + 1) * 128)
        xt = jnp.transpose(xbuf[me, sl, :])
        xti[0:width, sl] = xt
        xt = xt.astype(F32)
        half_sq.append(-0.5 * jnp.sum(xt * xt, axis=0, keepdims=True))
    half_sq = jnp.concatenate(half_sq, axis=0)
    abs_q = jnp.abs(live_q)
    log_q = jnp.where(abs_q > 0.0, jnp.log(jnp.where(abs_q > 0.0, abs_q, 1.0)) * float(width), NEG_BIG)
    hi, mid, low = split3(half_sq + log_q)
    sub16 = lax.broadcasted_iota(jnp.int32, (16, 128), 0)
    for grp in range(rows // 128):
        sl = slice(grp * 128, (grp + 1) * 128)
        row = slice(grp, grp + 1)
        piece = jnp.where(sub16 < 3, 1.0, jnp.where(sub16 == 3, hi[row], jnp.where(sub16 == 4, mid[row], jnp.where(
            sub16 == 5, low[row], 0.0))))
        xti[width:width + 16, sl] = piece.astype(BF16)
        cap[0:1, sl] = log_q[row]
    xti[width + 16:2 * width, :] = jnp.zeros((width - 16, rows), BF16)
    sacc[...] = jnp.zeros_like(sacc)
    tacc[...] = jnp.zeros_like(tacc)

    def build(parts):
        sub8 = lax.broadcasted_iota(jnp.int32, (8, 128), 0)
        for n, (blk, q) in enumerate(parts):
            for t in range(lanes_per):
                sl = slice((n * lanes_per + t) * 128, (n * lanes_per + t + 1) * 128)
                grp = q * lanes_per + t
                xt = jnp.transpose(xbuf[blk, pl.ds(pl.multiple_of(grp * 128, 128), 128), :])
                xjt[:, sl] = xt
                xt = xt.astype(F32)
                h, m, l = split3(-0.5 * jnp.sum(xt * xt, axis=0, keepdims=True))
                piece = jnp.where(sub8 == 0, h, jnp.where(sub8 == 1, m, jnp.where(sub8 == 2, l, jnp.where(
                    sub8 < 6, 1.0, 0.0))))
                piece = jnp.concatenate([piece, jnp.zeros((120, 128), F32)], axis=0)
                aug[sl, :] = jnp.transpose(piece).astype(BF16)
                cb[sl, :] = jnp.transpose(jnp.broadcast_to(aux[blk, pl.ds(grp, 1), :], (128, 128)))

    def compute(parts, own=False):
        build(parts)
        tiles = rows // TILE
        units = [(it, p) for it in range(tiles) for p in range(len(parts))]

        def gram(it, p):
            blk, q = parts[p]
            xj = xbuf[blk, pl.ds(pl.multiple_of(q * quarter, quarter), quarter), :]
            lhs = jnp.concatenate([xj, aug[p * quarter:(p + 1) * quarter, :]], axis=1)
            return jnp.dot(lhs, xti[:, it * TILE:(it + 1) * TILE], preferred_element_type=F32)

        grams = {}
        for unit in units[:LAG]:
            grams[unit] = gram(*unit)
        for idx, (it, p) in enumerate(units):
            sl = slice(it * TILE, (it + 1) * TILE)
            ps = slice(p * quarter, (p + 1) * quarter)
            if p == 0:
                ssum, tsum = sacc[:, sl], None
            charge = jnp.concatenate([cb[ps, :]] * (TILE // 128), axis=1)
            weight = jnp.exp2(jnp.minimum(grams.pop((it, p)), cap[0:1, sl]) * (LOG2E / width)) * charge
            if own and p == it:
                ri = lax.broadcasted_iota(jnp.int32, (TILE, TILE), 0)
                ci = lax.broadcasted_iota(jnp.int32, (TILE, TILE), 1)
                weight = jnp.where(ri == ci, 0.0, weight)
            for t in range(quarter // 8):
                ssum = ssum + weight[t * 8:(t + 1) * 8, :]
            if idx + LAG < len(units):
                grams[units[idx + LAG]] = gram(*units[idx + LAG])
            part = jnp.dot(xjt[:, ps], weight.astype(BF16), preferred_element_type=F32)
            tsum = part if tsum is None else tsum + part
            if p == len(parts) - 1:
                sacc[:, sl] = ssum
                tacc[:, sl] += tsum

    def wait_aux(slot, blocks=1):
        rcopy(aux.at[pl.ds(0, blocks)], aux.at[pl.ds(0, blocks)], aux_send, aux_recv.at[slot], partner).wait_recv()

    def start_aux(blk, slot, dev):
        rcopy(aux.at[blk], aux.at[blk], aux_send, aux_recv.at[slot], dev).start()

    with jax.named_scope('own'):
        compute([(me, q) for q in range(QUARTERS)], own=True)
    with jax.named_scope('partner_wait'):
        wait_aux(1)
        rcopy(xbuf.at[partner], xbuf.at[partner], row_send, recv_p, partner).wait_recv()
    with jax.named_scope('partner'):
        compute([(partner, q) for q in range(QUARTERS)])
    with jax.named_scope('aux_wait'):
        wait_aux(0, 2)
        start_aux(x_nbr, 2, partner)
        start_aux(y_nbr, 2, partner)
        start_aux(x_nbr, 3, y_nbr)

    def place(k):
        far = k // QUARTERS
        return (x_nbr + far * (diag - x_nbr), k % QUARTERS), (y_nbr + far * (diag - y_nbr), (k + 2) % QUARTERS)

    def pass_on(k):
        (blk_x, q_x), (blk_y, q_y) = place(k)
        src_x, src_y = qref(blk_x, q_x), qref(blk_y, q_y)
        rcopy(src_x, src_x, row_send, recv_x.at[k], partner).wait_recv()
        rcopy(src_x, src_x, row_send, prime.at[k], partner).start()

        @pl.when(k < 2)
        def _():
            rcopy(src_x, src_x, row_send, recv_x.at[k + QUARTERS], y_nbr).start()

        rcopy(src_y, src_y, row_send, recv_y.at[k], partner).wait_recv()
        rcopy(src_y, src_y, row_send, prime.at[k], partner).start()

        @pl.when(k < 2)
        def _():
            rcopy(src_y, src_y, row_send, recv_y.at[k + QUARTERS], x_nbr).start()

    with jax.named_scope('pass_on'):
        pass_on(0)

    @pl.loop(0, GROUPS)
    def _(k):
        @pl.when(k < GROUPS - 1)
        def _():
            with jax.named_scope('pass_on'):
                pass_on(k + 1)

        @pl.when(k == 0)
        def _():
            wait_aux(2, 2)

        @pl.when(k == QUARTERS - 1)
        def _():
            wait_aux(3)
            start_aux(diag, 4, partner)

        @pl.when(k == QUARTERS)
        def _():
            wait_aux(4)

        (blk_x, q_x), (blk_y, q_y) = place(k)
        pair = xbuf.at[0, pl.ds(0, 2 * quarter), :]
        with jax.named_scope('wait_prime'):
            rcopy(pair, pair, row_send, prime.at[k], partner).wait_recv()
        with jax.named_scope('group'):
            compute([(blk_x, q_x), (blk_y, q_y), (blk_x + off_p, q_x), (blk_y + off_p, q_y)])

    with jax.named_scope('share'):
        total = jnp.zeros((8, 128), F32)
        live_q = aux[me]
        sign = jnp.where(live_q < 0.0, -1.0, 1.0)
        for grp in range(rows // 128):
            total = total + sacc[:, grp * 128:(grp + 1) * 128] * sign[grp:grp + 1]
        share_ref[me] = total
    for n in range(1, 8):
        rcopy(share_ref.at[me], share_ref.at[me], e_send, e_recv, (me + n) % 8).start()
    with jax.named_scope('force'):
        for grp in range(rows // 128):
            sl = slice(grp * 128, (grp + 1) * 128)
            row_sum = jnp.sum(sacc[:, sl], axis=0, keepdims=True)
            force = (row_sum * xti[0:width, sl].astype(F32) - tacc[:, sl]) * (sign[grp:grp + 1] * (1.0 / width))
            force_ref[sl, :] = jnp.transpose(force)

    with jax.named_scope('tail'):
        others = share_ref.at[pl.ds(0, 7)]
        rcopy(others, others, e_send, e_recv, partner).wait()
        rcopy(aux.at[pl.ds(0, 7)], aux.at[pl.ds(0, 7)], aux_send, aux_recv.at[0], partner).wait_send()
        rcopy(xbuf.at[pl.ds(0, 7)], xbuf.at[pl.ds(0, 7)], row_send, recv_p, partner).wait_send()


def finish(force_ref, share_ref, force_hbm, energy_hbm, energy, sem):
    rows = force_ref.shape[0]
    copies = []
    for n in range(4):
        sl = pl.ds(n * (rows // 4), rows // 4)
        copies.append(pltpu.make_async_copy(force_ref.at[sl, :], force_hbm.at[sl, :], sem.at[n]))
    copies.append(pltpu.make_async_copy(energy, energy_hbm, sem.at[4]))
    for cp in copies[:4]:
        cp.start()
    energy[0] = 0.5 * jnp.sum(jnp.sum(share_ref[...], axis=0))
    copies[4].start()
    for cp in copies:
        cp.wait()


def solution(mesh):
    def per_device(positions, charges, counts):
        rows, width = positions.shape
        dma = pltpu.SemaphoreType.DMA
        vmem, hbm = pl.BlockSpec(memory_space=pltpu.VMEM), pl.BlockSpec(memory_space=pltpu.HBM)
        force_type = jax.ShapeDtypeStruct((rows, width), F32)
        forces, shares = pl.pallas_call(
            kernel,
            out_shape=(force_type, jax.ShapeDtypeStruct((8, 8, 128), F32)),
            in_specs=[hbm, hbm, hbm],
            out_specs=(vmem, vmem),
            scratch_shapes=[
                pltpu.VMEM((8, rows, width), BF16),
                pltpu.VMEM((8, 8, 128), F32),
                pltpu.VMEM((2 * width, rows), BF16),
                pltpu.VMEM((8, rows), F32),
                pltpu.VMEM((width, rows), BF16),
                pltpu.VMEM((rows, 128), BF16),
                pltpu.VMEM((rows, 128), F32),
                pltpu.VMEM((8, rows), F32),
                pltpu.VMEM((width, rows), F32),
                pltpu.VMEM((8, 128), F32),
                pltpu.SMEM((1,), jnp.int32),
                dma((3,)), dma, dma, dma((5,)), dma, dma((GROUPS,)), dma((GROUPS,)), dma((GROUPS,)), dma, dma,
            ],
            compiler_params=pltpu.CompilerParams(collective_id=0, has_side_effects=True, vmem_limit_bytes=VMEM_LIMIT),
        )(counts, pltpu.with_memory_space_constraint(positions, pltpu.HBM),
          pltpu.with_memory_space_constraint(charges.reshape(8, 128), pltpu.HBM))
        return pl.pallas_call(
            finish,
            out_shape=(force_type, jax.ShapeDtypeStruct((1,), F32)),
            in_specs=[vmem, vmem],
            out_specs=(hbm, hbm),
            scratch_shapes=[pltpu.SMEM((1,), F32), dma((5,))],
            compiler_params=pltpu.CompilerParams(vmem_limit_bytes=4 * 1024 * 1024),
        )(forces, shares)

    row_spec = P(('sys', 'row'), None)
    vec_spec = P(('sys', 'row'))
    return jax.shard_map(per_device, mesh=mesh, in_specs=(row_spec, vec_spec, vec_spec), out_specs=(row_spec, P('sys')),
                         check_vma=False)
```

```python
import jax
import jax.numpy as jnp
from jax import lax
from jax.experimental import pallas as pl
from jax.experimental.pallas import tpu as pltpu
from jax.sharding import PartitionSpec as P

F32, BF16 = jnp.float32, jnp.bfloat16
LOG2E = 1.4426950408889634
NEG_BIG = -1e30
QUARTERS = 4
GROUPS = 6
TILE = 512
LAG = 1
VMEM_LIMIT = 24 * 1024 * 1024


def split3(val):
    hi = val.astype(BF16).astype(F32)
    rest = val - hi
    mid = rest.astype(BF16).astype(F32)
    low = (rest - mid).astype(BF16).astype(F32)
    return hi, mid, low


def kernel(cnt_hbm, pos_hbm, q_hbm, force_ref, share_ref, xbuf, aux, xti, xtp, pacc, cap, xjt, aug, cb, sacc, tacc, qv, cnt,
           load_sem, row_send, aux_send, aux_recv, recv_p, recv_x, recv_y, prime, e_send, e_recv):
    rows, width = pos_hbm.shape
    quarter = rows // QUARTERS
    lanes_per = quarter // 128
    me = lax.axis_index('row')
    core, ax, ay = me % 2, (me // 2) % 2, me // 4
    off_p = 1 - 2 * core
    partner = me + off_p
    x_nbr = me + 2 - 4 * ax
    y_nbr = me + 4 - 8 * ay
    diag = x_nbr + 4 - 8 * ay

    def rcopy(src, dst, send, recv, dev):
        return pltpu.make_async_remote_copy(src_ref=src, dst_ref=dst, send_sem=send, recv_sem=recv,
                                            device_id={'row': dev}, device_id_type=pl.DeviceIdType.MESH)

    def qref(blk, q):
        return xbuf.at[blk, pl.ds(q * quarter, quarter), :]

    load = pltpu.make_async_copy(pos_hbm, xbuf.at[me], load_sem.at[0])
    load.start()
    load_q = pltpu.make_async_copy(q_hbm, qv, load_sem.at[1])
    load_q.start()
    load_c = pltpu.make_async_copy(cnt_hbm, cnt, load_sem.at[2])
    load_c.start()
    barrier = pltpu.get_barrier_semaphore()
    for dev in (partner, x_nbr, y_nbr):
        pl.semaphore_signal(barrier, inc=1, device_id={'row': dev}, device_id_type=pl.DeviceIdType.MESH)

    def send_quarter(k):
        rcopy(qref(me, k), qref(me, k), row_send, recv_x.at[k], x_nbr).start()
        qy = (k + 2) % QUARTERS
        rcopy(qref(me, qy), qref(me, qy), row_send, recv_y.at[k], y_nbr).start()

    load_q.wait()
    load_c.wait()
    row_id = lax.broadcasted_iota(jnp.int32, (8, 128), 0) * 128 + lax.broadcasted_iota(jnp.int32, (8, 128), 1)
    live_q = jnp.where(row_id < cnt[0], qv[...], 0.0)
    aux[me] = live_q
    load.wait()
    with jax.named_scope('bar_wait'):
        pl.semaphore_wait(barrier, 3)

    for slot, dev in ((0, x_nbr), (0, y_nbr), (1, partner)):
        rcopy(aux.at[me], aux.at[me], aux_send, aux_recv.at[slot], dev).start()
    send_quarter(0)
    rcopy(xbuf.at[me], xbuf.at[me], row_send, recv_p, partner).start()
    for k in range(1, QUARTERS):
        send_quarter(k)

    def fill_lanes(dst, blk, log_q):
        half_sq = []
        for grp in range(rows // 128):
            sl = slice(grp * 128, (grp + 1) * 128)
            xt = jnp.transpose(xbuf[blk, sl, :])
            dst[0:width, sl] = xt
            xt = xt.astype(F32)
            half_sq.append(-0.5 * jnp.sum(xt * xt, axis=0, keepdims=True))
        half_sq = jnp.concatenate(half_sq, axis=0)
        hi, mid, low = split3(half_sq if log_q is None else half_sq + log_q)
        sub16 = lax.broadcasted_iota(jnp.int32, (16, 128), 0)
        for grp in range(rows // 128):
            sl = slice(grp * 128, (grp + 1) * 128)
            row = slice(grp, grp + 1)
            piece = jnp.where(sub16 < 3, 1.0, jnp.where(sub16 == 3, hi[row], jnp.where(sub16 == 4, mid[row], jnp.where(
                sub16 == 5, low[row], 0.0))))
            dst[width:width + 16, sl] = piece.astype(BF16)

    abs_q = jnp.abs(live_q)
    log_q = jnp.where(abs_q > 0.0, jnp.log(jnp.where(abs_q > 0.0, abs_q, 1.0)) * float(width), NEG_BIG)
    fill_lanes(xti, me, log_q)
    for grp in range(rows // 128):
        cap[0:1, grp * 128:(grp + 1) * 128] = log_q[grp:grp + 1]
    for dst in (xti, xtp):
        dst[width + 16:2 * width, :] = jnp.zeros((width - 16, rows), BF16)
    sacc[...] = jnp.zeros_like(sacc)
    tacc[...] = jnp.zeros_like(tacc)

    def build(parts, pulls=True):
        sub8 = lax.broadcasted_iota(jnp.int32, (8, 128), 0)
        for n, (blk, q) in enumerate(parts):
            for t in range(lanes_per):
                sl = slice((n * lanes_per + t) * 128, (n * lanes_per + t + 1) * 128)
                grp = q * lanes_per + t
                xt = jnp.transpose(xbuf[blk, pl.ds(pl.multiple_of(grp * 128, 128), 128), :])
                if pulls:
                    xjt[:, sl] = xt
                xt = xt.astype(F32)
                h, m, l = split3(-0.5 * jnp.sum(xt * xt, axis=0, keepdims=True))
                piece = jnp.where(sub8 == 0, h, jnp.where(sub8 == 1, m, jnp.where(sub8 == 2, l, jnp.where(
                    sub8 < 6, 1.0, 0.0))))
                piece = jnp.concatenate([piece, jnp.zeros((120, 128), F32)], axis=0)
                aug[sl, :] = jnp.transpose(piece).astype(BF16)
                cb[sl, :] = jnp.transpose(jnp.broadcast_to(aux[blk, pl.ds(grp, 1), :], (128, 128)))

    def gram(parts, lanes, it, p):
        blk, q = parts[p]
        xj = xbuf[blk, pl.ds(pl.multiple_of(q * quarter, quarter), quarter), :]
        lhs = jnp.concatenate([xj, aug[p * quarter:(p + 1) * quarter, :]], axis=1)
        return jnp.dot(lhs, lanes[:, it * TILE:(it + 1) * TILE], preferred_element_type=F32)

    def compute(parts, own=False):
        build(parts)
        tiles = rows // TILE
        units = [(it, p) for p in range(len(parts)) for it in range(tiles)]
        grams = {}
        for unit in units[:LAG]:
            grams[unit] = gram(parts, xti, *unit)
        for idx, (it, p) in enumerate(units):
            sl = slice(it * TILE, (it + 1) * TILE)
            ps = slice(p * quarter, (p + 1) * quarter)
            ssum, tsum = sacc[:, sl], None
            charge = jnp.concatenate([cb[ps, :]] * (TILE // 128), axis=1)
            weight = jnp.exp2(jnp.minimum(grams.pop((it, p)), cap[0:1, sl]) * (LOG2E / width)) * charge
            if own and it * TILE <= p * quarter < (it + 1) * TILE:
                ri = lax.broadcasted_iota(jnp.int32, (quarter, TILE), 0) + (p * quarter - it * TILE)
                ci = lax.broadcasted_iota(jnp.int32, (quarter, TILE), 1)
                weight = jnp.where(ri == ci, 0.0, weight)
            for t in range(quarter // 8):
                ssum = ssum + weight[t * 8:(t + 1) * 8, :]
            if idx + LAG < len(units):
                grams[units[idx + LAG]] = gram(parts, xti, *units[idx + LAG])
            part = jnp.dot(xjt[:, ps], weight.astype(BF16), preferred_element_type=F32)
            tsum = part if tsum is None else tsum + part
            sacc[:, sl] = ssum
            tacc[:, sl] += tsum

    def pair_energy(row_blk, col_blk):
        fill_lanes(xtp, row_blk, None)
        parts = [(col_blk, q) for q in range(QUARTERS)]
        build(parts, pulls=False)
        for it in range(rows // TILE):
            psum = jnp.zeros((8, TILE), F32)
            for p in range(QUARTERS):
                charge = jnp.concatenate([cb[p * quarter:(p + 1) * quarter, :]] * (TILE // 128), axis=1)
                weight = jnp.exp2(jnp.minimum(gram(parts, xtp, it, p), 0.0) * (LOG2E / width)) * charge
                for t in range(quarter // 8):
                    psum = psum + weight[t * 8:(t + 1) * 8, :]
            pacc[:, it * TILE:(it + 1) * TILE] = psum
        total = jnp.zeros((8, 128), F32)
        for grp in range(rows // 128):
            total = total + pacc[:, grp * 128:(grp + 1) * 128] * aux[row_blk, grp:grp + 1, :]
        return total

    def send_share():
        total = 2.0 * pair_energy(x_nbr, y_nbr + ay * off_p)
        live_q = aux[me]
        for grp in range(rows // 128):
            signed = jnp.where(live_q[grp:grp + 1] < 0.0, -1.0, 1.0) * sacc[:, grp * 128:(grp + 1) * 128]
            total = total + signed
        share_ref[me] = total
        for n in range(1, 8):
            rcopy(share_ref.at[me], share_ref.at[me], e_send, e_recv, (me + n) % 8).start()

    def wait_aux(slot, blocks=1):
        rcopy(aux.at[pl.ds(0, blocks)], aux.at[pl.ds(0, blocks)], aux_send, aux_recv.at[slot], partner).wait_recv()

    def start_aux(blk, slot, dev):
        rcopy(aux.at[blk], aux.at[blk], aux_send, aux_recv.at[slot], dev).start()

    with jax.named_scope('own'):
        compute([(me, q) for q in range(QUARTERS)], own=True)
    with jax.named_scope('partner_wait'):
        wait_aux(1)
        rcopy(xbuf.at[partner], xbuf.at[partner], row_send, recv_p, partner).wait_recv()
    with jax.named_scope('partner'):
        compute([(partner, q) for q in range(QUARTERS)])
    with jax.named_scope('aux_wait'):
        wait_aux(0, 2)
        start_aux(x_nbr, 2, partner)
        start_aux(y_nbr, 2, partner)
        start_aux(x_nbr, 3, y_nbr)

    def place(k):
        far = k // QUARTERS
        return (x_nbr + far * (diag - x_nbr), k % QUARTERS), (y_nbr + far * (diag - y_nbr), (k + 2) % QUARTERS)

    def pass_on(k):
        (blk_x, q_x), (blk_y, q_y) = place(k)
        src_x, src_y = qref(blk_x, q_x), qref(blk_y, q_y)
        rcopy(src_x, src_x, row_send, recv_x.at[k], partner).wait_recv()
        rcopy(src_x, src_x, row_send, prime.at[k], partner).start()

        @pl.when(k < 2)
        def _():
            rcopy(src_x, src_x, row_send, recv_x.at[k + QUARTERS], y_nbr).start()

        rcopy(src_y, src_y, row_send, recv_y.at[k], partner).wait_recv()
        rcopy(src_y, src_y, row_send, prime.at[k], partner).start()

        @pl.when(k < 2)
        def _():
            rcopy(src_y, src_y, row_send, recv_y.at[k + QUARTERS], x_nbr).start()

    with jax.named_scope('pass_on'):
        pass_on(0)

    @pl.loop(0, GROUPS)
    def _(k):
        @pl.when(k == QUARTERS)
        def _():
            with jax.named_scope('energy'):
                send_share()

        @pl.when(k < GROUPS - 1)
        def _():
            with jax.named_scope('pass_on'):
                pass_on(k + 1)

        @pl.when(k == 0)
        def _():
            wait_aux(2, 2)

        @pl.when(k == QUARTERS - 1)
        def _():
            wait_aux(3)
            start_aux(diag, 4, partner)

        @pl.when(k == QUARTERS)
        def _():
            wait_aux(4)

        (blk_x, q_x), (blk_y, q_y) = place(k)
        pair = xbuf.at[0, pl.ds(0, 2 * quarter), :]
        with jax.named_scope('wait_prime'):
            rcopy(pair, pair, row_send, prime.at[k], partner).wait_recv()
        with jax.named_scope('group'):
            compute([(blk_x, q_x), (blk_y, q_y), (blk_x + off_p, q_x), (blk_y + off_p, q_y)])

    sign = jnp.where(aux[me] < 0.0, -1.0, 1.0)
    with jax.named_scope('force'):
        for grp in range(rows // 128):
            sl = slice(grp * 128, (grp + 1) * 128)
            row_sum = jnp.sum(sacc[:, sl], axis=0, keepdims=True)
            force = (row_sum * xti[0:width, sl].astype(F32) - tacc[:, sl]) * (sign[grp:grp + 1] * (1.0 / width))
            force_ref[sl, :] = jnp.transpose(force)

    with jax.named_scope('tail'):
        others = share_ref.at[pl.ds(0, 7)]
        rcopy(others, others, e_send, e_recv, partner).wait()
        rcopy(aux.at[pl.ds(0, 7)], aux.at[pl.ds(0, 7)], aux_send, aux_recv.at[0], partner).wait_send()
        rcopy(xbuf.at[pl.ds(0, 7)], xbuf.at[pl.ds(0, 7)], row_send, recv_p, partner).wait_send()


def finish(force_ref, share_ref, force_hbm, energy_hbm, energy, sem):
    rows = force_ref.shape[0]
    copies = []
    for n in range(4):
        sl = pl.ds(n * (rows // 4), rows // 4)
        copies.append(pltpu.make_async_copy(force_ref.at[sl, :], force_hbm.at[sl, :], sem.at[n]))
    copies.append(pltpu.make_async_copy(energy, energy_hbm, sem.at[4]))
    for cp in copies[:4]:
        cp.start()
    energy[0] = 0.5 * jnp.sum(jnp.sum(share_ref[...], axis=0))
    copies[4].start()
    for cp in copies:
        cp.wait()


def solution(mesh):
    def per_device(positions, charges, counts):
        rows, width = positions.shape
        dma = pltpu.SemaphoreType.DMA
        vmem, hbm = pl.BlockSpec(memory_space=pltpu.VMEM), pl.BlockSpec(memory_space=pltpu.HBM)
        force_type = jax.ShapeDtypeStruct((rows, width), F32)
        forces, shares = pl.pallas_call(
            kernel,
            out_shape=(force_type, jax.ShapeDtypeStruct((8, 8, 128), F32)),
            in_specs=[hbm, hbm, hbm],
            out_specs=(vmem, vmem),
            scratch_shapes=[
                pltpu.VMEM((8, rows, width), BF16),
                pltpu.VMEM((8, 8, 128), F32),
                pltpu.VMEM((2 * width, rows), BF16),
                pltpu.VMEM((2 * width, rows), BF16),
                pltpu.VMEM((8, rows), F32),
                pltpu.VMEM((8, rows), F32),
                pltpu.VMEM((width, rows), BF16),
                pltpu.VMEM((rows, 128), BF16),
                pltpu.VMEM((rows, 128), F32),
                pltpu.VMEM((8, rows), F32),
                pltpu.VMEM((width, rows), F32),
                pltpu.VMEM((8, 128), F32),
                pltpu.SMEM((1,), jnp.int32),
                dma((3,)), dma, dma, dma((5,)), dma, dma((GROUPS,)), dma((GROUPS,)), dma((GROUPS,)), dma, dma,
            ],
            compiler_params=pltpu.CompilerParams(collective_id=0, has_side_effects=True, vmem_limit_bytes=VMEM_LIMIT),
        )(counts, pltpu.with_memory_space_constraint(positions, pltpu.HBM),
          pltpu.with_memory_space_constraint(charges.reshape(8, 128), pltpu.HBM))
        return pl.pallas_call(
            finish,
            out_shape=(force_type, jax.ShapeDtypeStruct((1,), F32)),
            in_specs=[vmem, vmem],
            out_specs=(hbm, hbm),
            scratch_shapes=[pltpu.SMEM((1,), F32), dma((5,))],
            compiler_params=pltpu.CompilerParams(vmem_limit_bytes=4 * 1024 * 1024),
        )(forces, shares)

    row_spec = P(('sys', 'row'), None)
    vec_spec = P(('sys', 'row'))
    return jax.shard_map(per_device, mesh=mesh, in_specs=(row_spec, vec_spec, vec_spec), out_specs=(row_spec, P('sys')),
                         check_vma=False)
```

```python
import jax
import jax.numpy as jnp
from jax import lax
from jax.experimental import pallas as pl
from jax.experimental.pallas import tpu as pltpu
from jax.sharding import PartitionSpec as P

F32, BF16 = jnp.float32, jnp.bfloat16
LOG2E = 1.4426950408889634
NEG_BIG = -1e30
QUARTERS = 4
GROUPS = 6
TILE = 512
VMEM_LIMIT = 24 * 1024 * 1024


def split3(val):
    hi = val.astype(BF16).astype(F32)
    rest = val - hi
    mid = rest.astype(BF16).astype(F32)
    low = (rest - mid).astype(BF16).astype(F32)
    return hi, mid, low


def kernel(cnt_hbm, pos_hbm, q_hbm, force_ref, share_ref, xbuf, aux, xti, xtp, pacc, ptot, gpre, upre, aug_e, cb_e, cap, xjt, aug, cb, sacc, tacc, qv, cnt,
           load_sem, row_send, aux_send, aux_recv, recv_p, recv_x, recv_y, prime, e_send, e_recv):
    rows, width = pos_hbm.shape
    quarter = rows // QUARTERS
    lanes_per = quarter // 128
    me = lax.axis_index('row')
    core, ax, ay = me % 2, (me // 2) % 2, me // 4
    off_p = 1 - 2 * core
    partner = me + off_p
    x_nbr = me + 2 - 4 * ax
    y_nbr = me + 4 - 8 * ay
    diag = x_nbr + 4 - 8 * ay

    def rcopy(src, dst, send, recv, dev):
        return pltpu.make_async_remote_copy(src_ref=src, dst_ref=dst, send_sem=send, recv_sem=recv,
                                            device_id={'row': dev}, device_id_type=pl.DeviceIdType.MESH)

    def qref(blk, q):
        return xbuf.at[blk, pl.ds(q * quarter, quarter), :]

    load = pltpu.make_async_copy(pos_hbm, xbuf.at[me], load_sem.at[0])
    load.start()
    load_q = pltpu.make_async_copy(q_hbm, qv, load_sem.at[1])
    load_q.start()
    load_c = pltpu.make_async_copy(cnt_hbm, cnt, load_sem.at[2])
    load_c.start()
    barrier = pltpu.get_barrier_semaphore()
    for dev in (partner, x_nbr, y_nbr):
        pl.semaphore_signal(barrier, inc=1, device_id={'row': dev}, device_id_type=pl.DeviceIdType.MESH)

    def send_quarter(k):
        rcopy(qref(me, k), qref(me, k), row_send, recv_x.at[k], x_nbr).start()
        qy = (k + 2) % QUARTERS
        rcopy(qref(me, qy), qref(me, qy), row_send, recv_y.at[k], y_nbr).start()

    load_q.wait()
    load_c.wait()
    row_id = lax.broadcasted_iota(jnp.int32, (8, 128), 0) * 128 + lax.broadcasted_iota(jnp.int32, (8, 128), 1)
    live_q = jnp.where(row_id < cnt[0], qv[...], 0.0)
    aux[me] = live_q
    load.wait()
    with jax.named_scope('bar_wait'):
        pl.semaphore_wait(barrier, 3)

    for slot, dev in ((0, x_nbr), (0, y_nbr), (1, partner)):
        rcopy(aux.at[me], aux.at[me], aux_send, aux_recv.at[slot], dev).start()
    send_quarter(0)
    rcopy(xbuf.at[me], xbuf.at[me], row_send, recv_p, partner).start()
    for k in range(1, QUARTERS):
        send_quarter(k)

    def fill_lanes(dst, blk, log_q):
        half_sq = []
        for grp in range(rows // 128):
            sl = slice(grp * 128, (grp + 1) * 128)
            xt = jnp.transpose(xbuf[blk, sl, :])
            dst[0:width, sl] = xt
            xt = xt.astype(F32)
            half_sq.append(-0.5 * jnp.sum(xt * xt, axis=0, keepdims=True))
        half_sq = jnp.concatenate(half_sq, axis=0)
        hi, mid, low = split3(half_sq if log_q is None else half_sq + log_q)
        sub16 = lax.broadcasted_iota(jnp.int32, (16, 128), 0)
        for grp in range(rows // 128):
            sl = slice(grp * 128, (grp + 1) * 128)
            row = slice(grp, grp + 1)
            piece = jnp.where(sub16 < 3, 1.0, jnp.where(sub16 == 3, hi[row], jnp.where(sub16 == 4, mid[row], jnp.where(
                sub16 == 5, low[row], 0.0))))
            dst[width:width + 16, sl] = piece.astype(BF16)

    abs_q = jnp.abs(live_q)
    log_q = jnp.where(abs_q > 0.0, jnp.log(jnp.where(abs_q > 0.0, abs_q, 1.0)) * float(width), NEG_BIG)
    fill_lanes(xti, me, log_q)
    for grp in range(rows // 128):
        cap[0:1, grp * 128:(grp + 1) * 128] = log_q[grp:grp + 1]
    for dst in (xti, xtp):
        dst[width + 16:2 * width, :] = jnp.zeros((width - 16, rows), BF16)
    sacc[...] = jnp.zeros_like(sacc)
    tacc[...] = jnp.zeros_like(tacc)

    def build(parts, first=0, cols=None, charges=None, pulls=True):
        cols, charges = aug if cols is None else cols, cb if charges is None else charges
        sub8 = lax.broadcasted_iota(jnp.int32, (8, 128), 0)
        for n, (blk, q) in enumerate(parts):
            for t in range(lanes_per):
                start = ((first + n) * lanes_per + t) * 128
                sl = slice(start, start + 128)
                grp = q * lanes_per + t
                xt = jnp.transpose(xbuf[blk, pl.ds(pl.multiple_of(grp * 128, 128), 128), :])
                if pulls:
                    xjt[:, sl] = xt
                xt = xt.astype(F32)
                h, m, l = split3(-0.5 * jnp.sum(xt * xt, axis=0, keepdims=True))
                piece = jnp.where(sub8 == 0, h, jnp.where(sub8 == 1, m, jnp.where(sub8 == 2, l, jnp.where(
                    sub8 < 6, 1.0, 0.0))))
                piece = jnp.concatenate([piece, jnp.zeros((120, 128), F32)], axis=0)
                cols[sl, :] = jnp.transpose(piece).astype(BF16)
                charges[sl, :] = jnp.transpose(jnp.broadcast_to(aux[blk, pl.ds(grp, 1), :], (128, 128)))

    def gram(part, p, it, lanes=None, cols=None):
        lanes, cols = xti if lanes is None else lanes, aug if cols is None else cols
        blk, q = part
        xj = xbuf[blk, pl.ds(pl.multiple_of(q * quarter, quarter), quarter), :]
        lhs = jnp.concatenate([xj, cols[p * quarter:(p + 1) * quarter, :]], axis=1)
        return jnp.dot(lhs, lanes[:, it * TILE:(it + 1) * TILE], preferred_element_type=F32)

    tiles = rows // TILE
    units = [(p, it) for p in range(QUARTERS) for it in range(tiles)]
    last_p, last_it = units[-1]

    def pull(p, it, w_low):
        tacc[:, it * TILE:(it + 1) * TILE] += jnp.dot(xjt[:, p * quarter:(p + 1) * quarter], w_low,
                                                      preferred_element_type=F32)

    def weigh(p, it, product, own):
        sl = slice(it * TILE, (it + 1) * TILE)
        charge = jnp.concatenate([cb[p * quarter:(p + 1) * quarter, :]] * (TILE // 128), axis=1)
        weight = jnp.exp2(jnp.minimum(product, cap[0:1, sl]) * (LOG2E / width)) * charge
        if own and it * TILE <= p * quarter < (it + 1) * TILE:
            ri = lax.broadcasted_iota(jnp.int32, (quarter, TILE), 0) + (p * quarter - it * TILE)
            ci = lax.broadcasted_iota(jnp.int32, (quarter, TILE), 1)
            weight = jnp.where(ri == ci, 0.0, weight)
        ssum = sacc[:, sl]
        for t in range(quarter // 8):
            ssum = ssum + weight[t * 8:(t + 1) * 8, :]
        sacc[:, sl] = ssum
        return weight.astype(BF16)

    def compute(parts, own=False):
        build(parts)
        product = gram(parts[0], 0, 0)
        for idx, (p, it) in enumerate(units):
            w_low = weigh(p, it, product, own)
            if idx + 1 < len(units):
                n_p, n_it = units[idx + 1]
                product = gram(parts[n_p], n_p, n_it)
            pull(p, it, w_low)

    def start_trips(parts):
        build(parts)
        gpre[...] = gram(parts[0], 0, 0)
        upre[...] = jnp.zeros_like(upre)

    def trip(parts, next_parts):
        pull(last_p, last_it, upre[...])
        build(parts[2:], first=2)
        product = gpre[...]
        for idx, (p, it) in enumerate(units):
            w_low = weigh(p, it, product, False)
            if (p, it) == (1, tiles - 1):
                product = gram(parts[2], 2, 0)
                pull(p, it, w_low)
                build(next_parts)
            elif idx + 1 < len(units):
                n_p, n_it = units[idx + 1]
                product = gram(parts[n_p], n_p, n_it)
                pull(p, it, w_low)
            else:
                gpre[...] = gram(next_parts[0], 0, 0)
                upre[...] = w_low

    def pair_energy(row_blk, col_blk):
        fill_lanes(xtp, row_blk, None)
        parts = [(col_blk, q) for q in range(QUARTERS)]
        build(parts, cols=aug_e, charges=cb_e, pulls=False)
        for it in range(tiles):
            psum = jnp.zeros((8, TILE), F32)
            for p in range(QUARTERS):
                charge = jnp.concatenate([cb_e[p * quarter:(p + 1) * quarter, :]] * (TILE // 128), axis=1)
                product = gram(parts[p], p, it, lanes=xtp, cols=aug_e)
                weight = jnp.exp2(jnp.minimum(product, 0.0) * (LOG2E / width)) * charge
                for t in range(quarter // 8):
                    psum = psum + weight[t * 8:(t + 1) * 8, :]
            pacc[:, it * TILE:(it + 1) * TILE] = psum
        total = jnp.zeros((8, 128), F32)
        for grp in range(rows // 128):
            total = total + pacc[:, grp * 128:(grp + 1) * 128] * aux[row_blk, grp:grp + 1, :]
        ptot[...] = 2.0 * total

    def send_share():
        total = ptot[...]
        live_q = aux[me]
        for grp in range(rows // 128):
            signed = jnp.where(live_q[grp:grp + 1] < 0.0, -1.0, 1.0) * sacc[:, grp * 128:(grp + 1) * 128]
            total = total + signed
        share_ref[me] = total
        for n in range(1, 8):
            rcopy(share_ref.at[me], share_ref.at[me], e_send, e_recv, (me + n) % 8).start()

    def wait_aux(slot, blocks=1):
        rcopy(aux.at[pl.ds(0, blocks)], aux.at[pl.ds(0, blocks)], aux_send, aux_recv.at[slot], partner).wait_recv()

    def start_aux(blk, slot, dev):
        rcopy(aux.at[blk], aux.at[blk], aux_send, aux_recv.at[slot], dev).start()

    with jax.named_scope('own'):
        compute([(me, q) for q in range(QUARTERS)], own=True)
    with jax.named_scope('partner_wait'):
        wait_aux(1)
        rcopy(xbuf.at[partner], xbuf.at[partner], row_send, recv_p, partner).wait_recv()
    with jax.named_scope('partner'):
        compute([(partner, q) for q in range(QUARTERS)])
    with jax.named_scope('aux_wait'):
        wait_aux(0, 2)
        start_aux(x_nbr, 2, partner)
        start_aux(y_nbr, 2, partner)
        start_aux(x_nbr, 3, y_nbr)

    def place(k):
        far = k // QUARTERS
        return (x_nbr + far * (diag - x_nbr), k % QUARTERS), (y_nbr + far * (diag - y_nbr), (k + 2) % QUARTERS)

    def pass_on(k):
        (blk_x, q_x), (blk_y, q_y) = place(k)
        src_x, src_y = qref(blk_x, q_x), qref(blk_y, q_y)
        rcopy(src_x, src_x, row_send, recv_x.at[k], partner).wait_recv()
        rcopy(src_x, src_x, row_send, prime.at[k], partner).start()

        @pl.when(k < 2)
        def _():
            rcopy(src_x, src_x, row_send, recv_x.at[k + QUARTERS], y_nbr).start()

        rcopy(src_y, src_y, row_send, recv_y.at[k], partner).wait_recv()
        rcopy(src_y, src_y, row_send, prime.at[k], partner).start()

        @pl.when(k < 2)
        def _():
            rcopy(src_y, src_y, row_send, recv_y.at[k + QUARTERS], x_nbr).start()

    with jax.named_scope('pass_on'):
        pass_on(0)

    with jax.named_scope('start_trips'):
        start_trips(place(0))

    @pl.loop(0, GROUPS)
    def _(k):
        pair = xbuf.at[0, pl.ds(0, 2 * quarter), :]
        with jax.named_scope('wait_prime'):
            rcopy(pair, pair, row_send, prime.at[k], partner).wait_recv()

        @pl.when(k == 0)
        def _():
            wait_aux(2, 2)

        @pl.when(k == QUARTERS - 1)
        def _():
            with jax.named_scope('energy'):
                pair_energy(x_nbr, y_nbr + ay * off_p)

        @pl.when(k == QUARTERS)
        def _():
            with jax.named_scope('share'):
                send_share()

        @pl.when(k < GROUPS - 1)
        def _():
            with jax.named_scope('pass_on'):
                pass_on(k + 1)

        @pl.when(k == QUARTERS - 1)
        def _():
            wait_aux(3)
            start_aux(diag, 4, partner)

        @pl.when(k == QUARTERS)
        def _():
            wait_aux(4)

        (blk_x, q_x), (blk_y, q_y) = place(k)
        with jax.named_scope('group'):
            trip([(blk_x, q_x), (blk_y, q_y), (blk_x + off_p, q_x), (blk_y + off_p, q_y)],
                 place(k + 1 - (k + 1) // GROUPS))

    sign = jnp.where(aux[me] < 0.0, -1.0, 1.0)
    with jax.named_scope('force'):
        pull(last_p, last_it, upre[...])
        for grp in range(rows // 128):
            sl = slice(grp * 128, (grp + 1) * 128)
            row_sum = jnp.sum(sacc[:, sl], axis=0, keepdims=True)
            force = (row_sum * xti[0:width, sl].astype(F32) - tacc[:, sl]) * (sign[grp:grp + 1] * (1.0 / width))
            force_ref[sl, :] = jnp.transpose(force)

    with jax.named_scope('tail'):
        others = share_ref.at[pl.ds(0, 7)]
        rcopy(others, others, e_send, e_recv, partner).wait()
        rcopy(aux.at[pl.ds(0, 7)], aux.at[pl.ds(0, 7)], aux_send, aux_recv.at[0], partner).wait_send()
        rcopy(xbuf.at[pl.ds(0, 7)], xbuf.at[pl.ds(0, 7)], row_send, recv_p, partner).wait_send()


def finish(force_ref, share_ref, force_hbm, energy_hbm, energy, sem):
    rows = force_ref.shape[0]
    copies = []
    for n in range(4):
        sl = pl.ds(n * (rows // 4), rows // 4)
        copies.append(pltpu.make_async_copy(force_ref.at[sl, :], force_hbm.at[sl, :], sem.at[n]))
    copies.append(pltpu.make_async_copy(energy, energy_hbm, sem.at[4]))
    for cp in copies[:4]:
        cp.start()
    energy[0] = 0.5 * jnp.sum(jnp.sum(share_ref[...], axis=0))
    copies[4].start()
    for cp in copies:
        cp.wait()


def solution(mesh):
    def per_device(positions, charges, counts):
        rows, width = positions.shape
        dma = pltpu.SemaphoreType.DMA
        vmem, hbm = pl.BlockSpec(memory_space=pltpu.VMEM), pl.BlockSpec(memory_space=pltpu.HBM)
        force_type = jax.ShapeDtypeStruct((rows, width), F32)
        forces, shares = pl.pallas_call(
            kernel,
            out_shape=(force_type, jax.ShapeDtypeStruct((8, 8, 128), F32)),
            in_specs=[hbm, hbm, hbm],
            out_specs=(vmem, vmem),
            scratch_shapes=[
                pltpu.VMEM((8, rows, width), BF16),
                pltpu.VMEM((8, 8, 128), F32),
                pltpu.VMEM((2 * width, rows), BF16),
                pltpu.VMEM((2 * width, rows), BF16),
                pltpu.VMEM((8, rows), F32),
                pltpu.VMEM((8, 128), F32),
                pltpu.VMEM((rows // QUARTERS, TILE), F32),
                pltpu.VMEM((rows // QUARTERS, TILE), BF16),
                pltpu.VMEM((rows, 128), BF16),
                pltpu.VMEM((rows, 128), F32),
                pltpu.VMEM((8, rows), F32),
                pltpu.VMEM((width, rows), BF16),
                pltpu.VMEM((rows, 128), BF16),
                pltpu.VMEM((rows, 128), F32),
                pltpu.VMEM((8, rows), F32),
                pltpu.VMEM((width, rows), F32),
                pltpu.VMEM((8, 128), F32),
                pltpu.SMEM((1,), jnp.int32),
                dma((3,)), dma, dma, dma((5,)), dma, dma((GROUPS,)), dma((GROUPS,)), dma((GROUPS,)), dma, dma,
            ],
            compiler_params=pltpu.CompilerParams(collective_id=0, has_side_effects=True, vmem_limit_bytes=VMEM_LIMIT),
        )(counts, pltpu.with_memory_space_constraint(positions, pltpu.HBM),
          pltpu.with_memory_space_constraint(charges.reshape(8, 128), pltpu.HBM))
        return pl.pallas_call(
            finish,
            out_shape=(force_type, jax.ShapeDtypeStruct((1,), F32)),
            in_specs=[vmem, vmem],
            out_specs=(hbm, hbm),
            scratch_shapes=[pltpu.SMEM((1,), F32), dma((5,))],
            compiler_params=pltpu.CompilerParams(vmem_limit_bytes=4 * 1024 * 1024),
        )(forces, shares)

    row_spec = P(('sys', 'row'), None)
    vec_spec = P(('sys', 'row'))
    return jax.shard_map(per_device, mesh=mesh, in_specs=(row_spec, vec_spec, vec_spec), out_specs=(row_spec, P('sys')),
                         check_vma=False)
```

```python
import jax
import jax.numpy as jnp
from jax import lax
from jax.experimental import pallas as pl
from jax.experimental.pallas import tpu as pltpu
from jax.sharding import PartitionSpec as P

F32, BF16 = jnp.float32, jnp.bfloat16
LOG2E = 1.4426950408889634
NEG_BIG = -1e30
QUARTERS = 4
GROUPS = 6
TILE = 512
MIDDLE = 4
VMEM_LIMIT = 24 * 1024 * 1024


def split3(val):
    hi = val.astype(BF16).astype(F32)
    rest = val - hi
    mid = rest.astype(BF16).astype(F32)
    low = (rest - mid).astype(BF16).astype(F32)
    return hi, mid, low


def kernel(cnt_hbm, pos_hbm, q_hbm, force_ref, share_ref, xbuf, aux, xti, xtp, pacc, ptot, gpre, upre, aug_e, cb_e, cap, xjt, aug, cb, sacc, tacc, qv, cnt,
           load_sem, row_send, aux_send, aux_recv, recv_p, recv_g, prime, e_send, e_recv):
    rows, width = pos_hbm.shape
    quarter = rows // QUARTERS
    lanes_per = quarter // 128
    me = lax.axis_index('row')
    core, ax, ay = me % 2, (me // 2) % 2, me // 4
    off_p = 1 - 2 * core
    partner = me + off_p
    x_nbr = me + 2 - 4 * ax
    y_nbr = me + 4 - 8 * ay
    diag = x_nbr + 4 - 8 * ay

    def rcopy(src, dst, send, recv, dev):
        return pltpu.make_async_remote_copy(src_ref=src, dst_ref=dst, send_sem=send, recv_sem=recv,
                                            device_id={'row': dev}, device_id_type=pl.DeviceIdType.MESH)

    def qref(blk, q):
        return xbuf.at[blk, pl.ds(q * quarter, quarter), :]

    load = pltpu.make_async_copy(pos_hbm, xbuf.at[me], load_sem.at[0])
    load.start()
    load_q = pltpu.make_async_copy(q_hbm, qv, load_sem.at[1])
    load_q.start()
    load_c = pltpu.make_async_copy(cnt_hbm, cnt, load_sem.at[2])
    load_c.start()
    barrier = pltpu.get_barrier_semaphore()
    for dev in (partner, x_nbr, y_nbr):
        pl.semaphore_signal(barrier, inc=1, device_id={'row': dev}, device_id_type=pl.DeviceIdType.MESH)

    def send_quarter(k):
        rcopy(qref(me, k), qref(me, k), row_send, recv_g.at[k], x_nbr).start()
        qy = (k + 2) % QUARTERS
        rcopy(qref(me, qy), qref(me, qy), row_send, recv_g.at[k], y_nbr).start()

    load_q.wait()
    load_c.wait()
    row_id = lax.broadcasted_iota(jnp.int32, (8, 128), 0) * 128 + lax.broadcasted_iota(jnp.int32, (8, 128), 1)
    live_q = jnp.where(row_id < cnt[0], qv[...], 0.0)
    aux[me] = live_q
    load.wait()
    with jax.named_scope('bar_wait'):
        pl.semaphore_wait(barrier, 3)

    for slot, dev in ((0, x_nbr), (0, y_nbr), (1, partner)):
        rcopy(aux.at[me], aux.at[me], aux_send, aux_recv.at[slot], dev).start()
    send_quarter(0)
    rcopy(xbuf.at[me], xbuf.at[me], row_send, recv_p, partner).start()
    for k in range(1, QUARTERS):
        send_quarter(k)

    def fill_lanes(dst, blk, log_q):
        half_sq = []
        for grp in range(rows // 128):
            sl = slice(grp * 128, (grp + 1) * 128)
            xt = jnp.transpose(xbuf[blk, sl, :])
            dst[0:width, sl] = xt
            xt = xt.astype(F32)
            half_sq.append(-0.5 * jnp.sum(xt * xt, axis=0, keepdims=True))
        half_sq = jnp.concatenate(half_sq, axis=0)
        hi, mid, low = split3(half_sq if log_q is None else half_sq + log_q)
        sub16 = lax.broadcasted_iota(jnp.int32, (16, 128), 0)
        for grp in range(rows // 128):
            sl = slice(grp * 128, (grp + 1) * 128)
            row = slice(grp, grp + 1)
            piece = jnp.where(sub16 < 3, 1.0, jnp.where(sub16 == 3, hi[row], jnp.where(sub16 == 4, mid[row], jnp.where(
                sub16 == 5, low[row], 0.0))))
            dst[width:width + 16, sl] = piece.astype(BF16)

    abs_q = jnp.abs(live_q)
    log_q = jnp.where(abs_q > 0.0, jnp.log(jnp.where(abs_q > 0.0, abs_q, 1.0)) * float(width), NEG_BIG)
    fill_lanes(xti, me, log_q)
    for grp in range(rows // 128):
        cap[0:1, grp * 128:(grp + 1) * 128] = log_q[grp:grp + 1]
    for dst in (xti, xtp):
        dst[width + 16:2 * width, :] = jnp.zeros((width - 16, rows), BF16)
    sacc[...] = jnp.zeros_like(sacc)
    tacc[...] = jnp.zeros_like(tacc)

    def build(parts, first=0, cols=None, charges=None, pulls=True):
        cols, charges = aug if cols is None else cols, cb if charges is None else charges
        sub8 = lax.broadcasted_iota(jnp.int32, (8, 128), 0)
        for n, (blk, q) in enumerate(parts):
            for t in range(lanes_per):
                start = ((first + n) * lanes_per + t) * 128
                sl = slice(start, start + 128)
                grp = q * lanes_per + t
                xt = jnp.transpose(xbuf[blk, pl.ds(pl.multiple_of(grp * 128, 128), 128), :])
                if pulls:
                    xjt[:, sl] = xt
                xt = xt.astype(F32)
                h, m, l = split3(-0.5 * jnp.sum(xt * xt, axis=0, keepdims=True))
                piece = jnp.where(sub8 == 0, h, jnp.where(sub8 == 1, m, jnp.where(sub8 == 2, l, jnp.where(
                    sub8 < 6, 1.0, 0.0))))
                piece = jnp.concatenate([piece, jnp.zeros((120, 128), F32)], axis=0)
                cols[sl, :] = jnp.transpose(piece).astype(BF16)
                charges[sl, :] = jnp.transpose(jnp.broadcast_to(aux[blk, pl.ds(grp, 1), :], (128, 128)))

    def gram(part, p, it, lanes=None, cols=None):
        lanes, cols = xti if lanes is None else lanes, aug if cols is None else cols
        blk, q = part
        xj = xbuf[blk, pl.ds(pl.multiple_of(q * quarter, quarter), quarter), :]
        lhs = jnp.concatenate([xj, cols[p * quarter:(p + 1) * quarter, :]], axis=1)
        return jnp.dot(lhs, lanes[:, it * TILE:(it + 1) * TILE], preferred_element_type=F32)

    tiles = rows // TILE
    units = [(p, it) for p in range(QUARTERS) for it in range(tiles)]
    last_p, last_it = units[-1]

    def pull(p, it, w_low):
        tacc[:, it * TILE:(it + 1) * TILE] += jnp.dot(xjt[:, p * quarter:(p + 1) * quarter], w_low,
                                                      preferred_element_type=F32)

    def weigh(p, it, product, own):
        sl = slice(it * TILE, (it + 1) * TILE)
        charge = jnp.concatenate([cb[p * quarter:(p + 1) * quarter, :]] * (TILE // 128), axis=1)
        weight = jnp.exp2(jnp.minimum(product, cap[0:1, sl]) * (LOG2E / width)) * charge
        if own and it * TILE <= p * quarter < (it + 1) * TILE:
            ri = lax.broadcasted_iota(jnp.int32, (quarter, TILE), 0) + (p * quarter - it * TILE)
            ci = lax.broadcasted_iota(jnp.int32, (quarter, TILE), 1)
            weight = jnp.where(ri == ci, 0.0, weight)
        ssum = sacc[:, sl]
        for t in range(quarter // 8):
            ssum = ssum + weight[t * 8:(t + 1) * 8, :]
        sacc[:, sl] = ssum
        return weight.astype(BF16)

    def compute(parts, own=False):
        build(parts)
        product = gram(parts[0], 0, 0)
        for idx, (p, it) in enumerate(units):
            w_low = weigh(p, it, product, own)
            if idx + 1 < len(units):
                n_p, n_it = units[idx + 1]
                product = gram(parts[n_p], n_p, n_it)
            pull(p, it, w_low)

    def start_trips(parts):
        build(parts)
        gpre[...] = gram(parts[0], 0, 0)
        upre[...] = jnp.zeros_like(upre)

    def trip(parts, next_parts=None, between=None):
        pull(last_p, last_it, upre[...])
        build(parts[2:], first=2)
        product = gpre[...]
        for idx, (p, it) in enumerate(units):
            w_low = weigh(p, it, product, False)
            if idx + 1 < len(units):
                n_p, n_it = units[idx + 1]
                product = gram(parts[n_p], n_p, n_it)
                pull(p, it, w_low)
            elif next_parts is None:
                pull(p, it, w_low)
            else:
                gpre[...] = gram(next_parts[0], 0, 0)
                upre[...] = w_low
            if idx == MIDDLE and next_parts is not None:
                between()
                build(next_parts)

    def pair_energy(row_blk, col_blk):
        fill_lanes(xtp, row_blk, None)
        parts = [(col_blk, q) for q in range(QUARTERS)]
        build(parts, cols=aug_e, charges=cb_e, pulls=False)
        for it in range(tiles):
            psum = jnp.zeros((8, TILE), F32)
            for p in range(QUARTERS):
                charge = jnp.concatenate([cb_e[p * quarter:(p + 1) * quarter, :]] * (TILE // 128), axis=1)
                product = gram(parts[p], p, it, lanes=xtp, cols=aug_e)
                weight = jnp.exp2(jnp.minimum(product, 0.0) * (LOG2E / width)) * charge
                for t in range(quarter // 8):
                    psum = psum + weight[t * 8:(t + 1) * 8, :]
            pacc[:, it * TILE:(it + 1) * TILE] = psum
        total = jnp.zeros((8, 128), F32)
        for grp in range(rows // 128):
            total = total + pacc[:, grp * 128:(grp + 1) * 128] * aux[row_blk, grp:grp + 1, :]
        ptot[...] = 2.0 * total

    def send_share():
        total = ptot[...]
        live_q = aux[me]
        for grp in range(rows // 128):
            signed = jnp.where(live_q[grp:grp + 1] < 0.0, -1.0, 1.0) * sacc[:, grp * 128:(grp + 1) * 128]
            total = total + signed
        share_ref[me] = total
        for n in range(1, 8):
            rcopy(share_ref.at[me], share_ref.at[me], e_send, e_recv, (me + n) % 8).start()

    pair = xbuf.at[0, pl.ds(0, 2 * quarter), :]

    def wait_aux(slot, blocks=1):
        rcopy(aux.at[pl.ds(0, blocks)], aux.at[pl.ds(0, blocks)], aux_send, aux_recv.at[slot], partner).wait_recv()

    def start_aux(blk, slot, dev):
        rcopy(aux.at[blk], aux.at[blk], aux_send, aux_recv.at[slot], dev).start()

    with jax.named_scope('own'):
        compute([(me, q) for q in range(QUARTERS)], own=True)
    with jax.named_scope('partner_wait'):
        wait_aux(1)
        rcopy(xbuf.at[partner], xbuf.at[partner], row_send, recv_p, partner).wait_recv()
    with jax.named_scope('partner'):
        compute([(partner, q) for q in range(QUARTERS)])
    with jax.named_scope('aux_wait'):
        wait_aux(0, 2)
        start_aux(x_nbr, 2, partner)
        start_aux(y_nbr, 2, partner)
        start_aux(x_nbr, 3, y_nbr)

    def place(k):
        far = k // QUARTERS
        return (x_nbr + far * (diag - x_nbr), k % QUARTERS), (y_nbr + far * (diag - y_nbr), (k + 2) % QUARTERS)

    def pass_on(k):
        (blk_x, q_x), (blk_y, q_y) = place(k)
        src_x, src_y = qref(blk_x, q_x), qref(blk_y, q_y)
        rcopy(pair, pair, row_send, recv_g.at[k], partner).wait_recv()

        @pl.when(k < 2)
        def _():
            rcopy(src_x, src_x, row_send, recv_g.at[k + QUARTERS], y_nbr).start()
            rcopy(src_y, src_y, row_send, recv_g.at[k + QUARTERS], x_nbr).start()

        for src in (src_x, src_y):
            rcopy(src, src, row_send, prime.at[k], partner).start()

    with jax.named_scope('pass_on'):
        pass_on(0)

    with jax.named_scope('start_trips'):
        start_trips(place(0))

    with jax.named_scope('start_trips'):
        start_trips(place(0))

    def whole(k):
        (blk_x, q_x), (blk_y, q_y) = place(k)
        return [(blk_x, q_x), (blk_y, q_y), (blk_x + off_p, q_x), (blk_y + off_p, q_y)]

    def wait_prime(k):
        with jax.named_scope('wait_prime'):
            rcopy(pair, pair, row_send, prime.at[k], partner).wait_recv()

    @pl.loop(0, GROUPS - 1)
    def _(k):
        wait_prime(k)

        @pl.when(k == 0)
        def _():
            wait_aux(2, 2)

        @pl.when(k == QUARTERS - 1)
        def _():
            with jax.named_scope('energy'):
                pair_energy(x_nbr, y_nbr + ay * off_p)
            wait_aux(3)
            start_aux(diag, 4, partner)

        @pl.when(k == QUARTERS)
        def _():
            with jax.named_scope('share'):
                send_share()
            wait_aux(4)

        with jax.named_scope('group'):
            trip(whole(k), place(k + 1), lambda: pass_on(k + 1))

    wait_prime(GROUPS - 1)
    with jax.named_scope('group'):
        trip(whole(GROUPS - 1))

    sign = jnp.where(aux[me] < 0.0, -1.0, 1.0)
    with jax.named_scope('force'):
        for grp in range(rows // 128):
            sl = slice(grp * 128, (grp + 1) * 128)
            row_sum = jnp.sum(sacc[:, sl], axis=0, keepdims=True)
            force = (row_sum * xti[0:width, sl].astype(F32) - tacc[:, sl]) * (sign[grp:grp + 1] * (1.0 / width))
            force_ref[sl, :] = jnp.transpose(force)

    with jax.named_scope('tail'):
        others = share_ref.at[pl.ds(0, 7)]
        rcopy(others, others, e_send, e_recv, partner).wait()
        rcopy(aux.at[pl.ds(0, 7)], aux.at[pl.ds(0, 7)], aux_send, aux_recv.at[0], partner).wait_send()
        rcopy(xbuf.at[pl.ds(0, 7)], xbuf.at[pl.ds(0, 7)], row_send, recv_p, partner).wait_send()


def finish(force_ref, share_ref, force_hbm, energy_hbm, energy, sem):
    rows = force_ref.shape[0]
    copies = []
    for n in range(4):
        sl = pl.ds(n * (rows // 4), rows // 4)
        copies.append(pltpu.make_async_copy(force_ref.at[sl, :], force_hbm.at[sl, :], sem.at[n]))
    copies.append(pltpu.make_async_copy(energy, energy_hbm, sem.at[4]))
    for cp in copies[:4]:
        cp.start()
    energy[0] = 0.5 * jnp.sum(jnp.sum(share_ref[...], axis=0))
    copies[4].start()
    for cp in copies:
        cp.wait()


def solution(mesh):
    def per_device(positions, charges, counts):
        rows, width = positions.shape
        dma = pltpu.SemaphoreType.DMA
        vmem, hbm = pl.BlockSpec(memory_space=pltpu.VMEM), pl.BlockSpec(memory_space=pltpu.HBM)
        force_type = jax.ShapeDtypeStruct((rows, width), F32)
        forces, shares = pl.pallas_call(
            kernel,
            out_shape=(force_type, jax.ShapeDtypeStruct((8, 8, 128), F32)),
            in_specs=[hbm, hbm, hbm],
            out_specs=(vmem, vmem),
            scratch_shapes=[
                pltpu.VMEM((8, rows, width), BF16),
                pltpu.VMEM((8, 8, 128), F32),
                pltpu.VMEM((2 * width, rows), BF16),
                pltpu.VMEM((2 * width, rows), BF16),
                pltpu.VMEM((8, rows), F32),
                pltpu.VMEM((8, 128), F32),
                pltpu.VMEM((rows // QUARTERS, TILE), F32),
                pltpu.VMEM((rows // QUARTERS, TILE), BF16),
                pltpu.VMEM((rows, 128), BF16),
                pltpu.VMEM((rows, 128), F32),
                pltpu.VMEM((8, rows), F32),
                pltpu.VMEM((width, rows), BF16),
                pltpu.VMEM((rows, 128), BF16),
                pltpu.VMEM((rows, 128), F32),
                pltpu.VMEM((8, rows), F32),
                pltpu.VMEM((width, rows), F32),
                pltpu.VMEM((8, 128), F32),
                pltpu.SMEM((1,), jnp.int32),
                dma((3,)), dma, dma, dma((5,)), dma, dma((GROUPS,)), dma((GROUPS,)), dma, dma,
            ],
            compiler_params=pltpu.CompilerParams(collective_id=0, has_side_effects=True, vmem_limit_bytes=VMEM_LIMIT),
        )(counts, pltpu.with_memory_space_constraint(positions, pltpu.HBM),
          pltpu.with_memory_space_constraint(charges.reshape(8, 128), pltpu.HBM))
        return pl.pallas_call(
            finish,
            out_shape=(force_type, jax.ShapeDtypeStruct((1,), F32)),
            in_specs=[vmem, vmem],
            out_specs=(hbm, hbm),
            scratch_shapes=[pltpu.SMEM((1,), F32), dma((5,))],
            compiler_params=pltpu.CompilerParams(vmem_limit_bytes=4 * 1024 * 1024),
        )(forces, shares)

    row_spec = P(('sys', 'row'), None)
    vec_spec = P(('sys', 'row'))
    return jax.shard_map(per_device, mesh=mesh, in_specs=(row_spec, vec_spec, vec_spec), out_specs=(row_spec, P('sys')),
                         check_vma=False)
```

```python
import jax
import jax.numpy as jnp
from jax import lax
from jax.experimental import pallas as pl
from jax.experimental.pallas import tpu as pltpu
from jax.sharding import PartitionSpec as P

F32, BF16 = jnp.float32, jnp.bfloat16
LOG2E = 1.4426950408889634
NEG_BIG = -1e30
QUARTERS = 4
GROUPS = 6
TILE = 512
VMEM_LIMIT = 24 * 1024 * 1024


def split3(val):
    hi = val.astype(BF16).astype(F32)
    rest = val - hi
    mid = rest.astype(BF16).astype(F32)
    low = (rest - mid).astype(BF16).astype(F32)
    return hi, mid, low


def kernel(cnt_hbm, pos_hbm, q_hbm, force_ref, share_ref, xbuf, aux, xti, xtp, pacc, ptot, gpre, upre, aug_e, cb_e, cap, xjt, aug, cb, sacc, tacc, qv, cnt,
           load_sem, row_send, aux_send, aux_recv, recv_p, recv_x, recv_y, prime, e_send, e_recv):
    rows, width = pos_hbm.shape
    quarter = rows // QUARTERS
    lanes_per = quarter // 128
    me = lax.axis_index('row')
    core, ax, ay = me % 2, (me // 2) % 2, me // 4
    off_p = 1 - 2 * core
    partner = me + off_p
    x_nbr = me + 2 - 4 * ax
    y_nbr = me + 4 - 8 * ay
    diag = x_nbr + 4 - 8 * ay

    def rcopy(src, dst, send, recv, dev):
        return pltpu.make_async_remote_copy(src_ref=src, dst_ref=dst, send_sem=send, recv_sem=recv,
                                            device_id={'row': dev}, device_id_type=pl.DeviceIdType.MESH)

    def qref(blk, q):
        return xbuf.at[blk, pl.ds(q * quarter, quarter), :]

    load = pltpu.make_async_copy(pos_hbm, xbuf.at[me], load_sem.at[0])
    load.start()
    load_q = pltpu.make_async_copy(q_hbm, qv, load_sem.at[1])
    load_q.start()
    load_c = pltpu.make_async_copy(cnt_hbm, cnt, load_sem.at[2])
    load_c.start()
    barrier = pltpu.get_barrier_semaphore()
    for dev in (partner, x_nbr, y_nbr):
        pl.semaphore_signal(barrier, inc=1, device_id={'row': dev}, device_id_type=pl.DeviceIdType.MESH)

    def send_quarter(k):
        rcopy(qref(me, k), qref(me, k), row_send, recv_x.at[k], x_nbr).start()
        qy = (k + 2) % QUARTERS
        rcopy(qref(me, qy), qref(me, qy), row_send, recv_y.at[k], y_nbr).start()

    load_q.wait()
    load_c.wait()
    row_id = lax.broadcasted_iota(jnp.int32, (8, 128), 0) * 128 + lax.broadcasted_iota(jnp.int32, (8, 128), 1)
    live_q = jnp.where(row_id < cnt[0], qv[...], 0.0)
    aux[me, 0:8, :] = live_q
    load.wait()
    with jax.named_scope('bar_wait'):
        pl.semaphore_wait(barrier, 3)

    send_quarter(0)

    def fill_lanes(dst, blk, log_q):
        half_sq = []
        for grp in range(rows // 128):
            sl = slice(grp * 128, (grp + 1) * 128)
            xt = jnp.transpose(xbuf[blk, sl, :])
            dst[0:width, sl] = xt
            if log_q is not None:
                xt = xt.astype(F32)
                half_sq.append(-0.5 * jnp.sum(xt * xt, axis=0, keepdims=True))
        if log_q is None:
            half_sq = aux[blk, 8:16, :]
        else:
            half_sq = jnp.concatenate(half_sq, axis=0)
            aux[blk, 8:16, :] = half_sq
        hi, mid, low = split3(half_sq if log_q is None else half_sq + log_q)
        sub16 = lax.broadcasted_iota(jnp.int32, (16, 128), 0)
        for grp in range(rows // 128):
            sl = slice(grp * 128, (grp + 1) * 128)
            row = slice(grp, grp + 1)
            piece = jnp.where(sub16 < 3, 1.0, jnp.where(sub16 == 3, hi[row], jnp.where(sub16 == 4, mid[row], jnp.where(
                sub16 == 5, low[row], 0.0))))
            dst[width:width + 16, sl] = piece.astype(BF16)

    abs_q = jnp.abs(live_q)
    log_q = jnp.where(abs_q > 0.0, jnp.log(jnp.where(abs_q > 0.0, abs_q, 1.0)) * float(width), NEG_BIG)
    fill_lanes(xti, me, log_q)
    for grp in range(rows // 128):
        cap[0:1, grp * 128:(grp + 1) * 128] = log_q[grp:grp + 1]
    for dst in (xti, xtp):
        dst[width + 16:2 * width, :] = jnp.zeros((width - 16, rows), BF16)
    for slot, dev in ((0, x_nbr), (0, y_nbr), (1, partner)):
        rcopy(aux.at[me], aux.at[me], aux_send, aux_recv.at[slot], dev).start()
    rcopy(xbuf.at[me], xbuf.at[me], row_send, recv_p, partner).start()
    for k in range(1, QUARTERS):
        send_quarter(k)
    sacc[...] = jnp.zeros_like(sacc)
    tacc[...] = jnp.zeros_like(tacc)

    def build(parts, first=0, cols=None, charges=None, pulls=True):
        cols, charges = aug if cols is None else cols, cb if charges is None else charges
        sub8 = lax.broadcasted_iota(jnp.int32, (8, 128), 0)
        for n, (blk, q) in enumerate(parts):
            for t in range(lanes_per):
                start = ((first + n) * lanes_per + t) * 128
                sl = slice(start, start + 128)
                grp = q * lanes_per + t
                if pulls:
                    xjt[:, sl] = jnp.transpose(xbuf[blk, pl.ds(pl.multiple_of(grp * 128, 128), 128), :])
                h, m, l = split3(aux[blk, pl.ds(8 + grp, 1), :])
                piece = jnp.where(sub8 == 0, h, jnp.where(sub8 == 1, m, jnp.where(sub8 == 2, l, jnp.where(
                    sub8 < 6, 1.0, 0.0))))
                piece = jnp.concatenate([piece, jnp.zeros((120, 128), F32)], axis=0)
                cols[sl, :] = jnp.transpose(piece).astype(BF16)
                charges[sl, :] = jnp.transpose(jnp.broadcast_to(aux[blk, pl.ds(grp, 1), :], (128, 128)))

    def gram(part, p, it, lanes=None, cols=None):
        lanes, cols = xti if lanes is None else lanes, aug if cols is None else cols
        blk, q = part
        xj = xbuf[blk, pl.ds(pl.multiple_of(q * quarter, quarter), quarter), :]
        lhs = jnp.concatenate([xj, cols[p * quarter:(p + 1) * quarter, :]], axis=1)
        return jnp.dot(lhs, lanes[:, it * TILE:(it + 1) * TILE], preferred_element_type=F32)

    tiles = rows // TILE
    units = [(p, it) for p in range(QUARTERS) for it in range(tiles)]
    last_p, last_it = units[-1]

    def pull(p, it, w_low):
        tacc[:, it * TILE:(it + 1) * TILE] += jnp.dot(xjt[:, p * quarter:(p + 1) * quarter], w_low,
                                                      preferred_element_type=F32)

    def weigh(p, it, product, own):
        sl = slice(it * TILE, (it + 1) * TILE)
        charge = jnp.concatenate([cb[p * quarter:(p + 1) * quarter, :]] * (TILE // 128), axis=1)
        weight = jnp.exp2(jnp.minimum(product, cap[0:1, sl]) * (LOG2E / width)) * charge
        if own and it * TILE <= p * quarter < (it + 1) * TILE:
            ri = lax.broadcasted_iota(jnp.int32, (quarter, TILE), 0) + (p * quarter - it * TILE)
            ci = lax.broadcasted_iota(jnp.int32, (quarter, TILE), 1)
            weight = jnp.where(ri == ci, 0.0, weight)
        ssum = sacc[:, sl]
        for t in range(quarter // 8):
            ssum = ssum + weight[t * 8:(t + 1) * 8, :]
        sacc[:, sl] = ssum
        return weight.astype(BF16)

    def compute(parts, own=False):
        build(parts)
        product = gram(parts[0], 0, 0)
        for idx, (p, it) in enumerate(units):
            w_low = weigh(p, it, product, own)
            if idx + 1 < len(units):
                n_p, n_it = units[idx + 1]
                product = gram(parts[n_p], n_p, n_it)
            pull(p, it, w_low)

    def start_trips(parts):
        build(parts)
        gpre[...] = gram(parts[0], 0, 0)
        upre[...] = jnp.zeros_like(upre)

    def trip(parts, next_parts):
        pull(last_p, last_it, upre[...])
        build(parts[2:], first=2)
        product = gpre[...]
        for idx, (p, it) in enumerate(units):
            w_low = weigh(p, it, product, False)
            if (p, it) == (1, tiles - 1):
                product = gram(parts[2], 2, 0)
                pull(p, it, w_low)
                build(next_parts)
            elif idx + 1 < len(units):
                n_p, n_it = units[idx + 1]
                product = gram(parts[n_p], n_p, n_it)
                pull(p, it, w_low)
            else:
                gpre[...] = gram(next_parts[0], 0, 0)
                upre[...] = w_low

    def pair_energy(row_blk, col_blk):
        fill_lanes(xtp, row_blk, None)
        parts = [(col_blk, q) for q in range(QUARTERS)]
        build(parts, cols=aug_e, charges=cb_e, pulls=False)
        for it in range(tiles):
            psum = jnp.zeros((8, TILE), F32)
            for p in range(QUARTERS):
                charge = jnp.concatenate([cb_e[p * quarter:(p + 1) * quarter, :]] * (TILE // 128), axis=1)
                product = gram(parts[p], p, it, lanes=xtp, cols=aug_e)
                weight = jnp.exp2(jnp.minimum(product, 0.0) * (LOG2E / width)) * charge
                for t in range(quarter // 8):
                    psum = psum + weight[t * 8:(t + 1) * 8, :]
            pacc[:, it * TILE:(it + 1) * TILE] = psum
        total = jnp.zeros((8, 128), F32)
        for grp in range(rows // 128):
            total = total + pacc[:, grp * 128:(grp + 1) * 128] * aux[row_blk, grp:grp + 1, :]
        ptot[...] = 2.0 * total

    def send_share():
        total = ptot[...]
        live_q = aux[me, 0:8, :]
        for grp in range(rows // 128):
            signed = jnp.where(live_q[grp:grp + 1] < 0.0, -1.0, 1.0) * sacc[:, grp * 128:(grp + 1) * 128]
            total = total + signed
        share_ref[me] = total
        for n in range(1, 8):
            rcopy(share_ref.at[me], share_ref.at[me], e_send, e_recv, (me + n) % 8).start()

    def wait_aux(slot, blocks=1):
        rcopy(aux.at[pl.ds(0, blocks)], aux.at[pl.ds(0, blocks)], aux_send, aux_recv.at[slot], partner).wait_recv()

    def start_aux(blk, slot, dev):
        rcopy(aux.at[blk], aux.at[blk], aux_send, aux_recv.at[slot], dev).start()

    with jax.named_scope('own'):
        compute([(me, q) for q in range(QUARTERS)], own=True)
    with jax.named_scope('partner_wait'):
        wait_aux(1)
        rcopy(xbuf.at[partner], xbuf.at[partner], row_send, recv_p, partner).wait_recv()
    with jax.named_scope('partner'):
        compute([(partner, q) for q in range(QUARTERS)])
    def place(k):
        far = k // QUARTERS
        return (x_nbr + far * (diag - x_nbr), k % QUARTERS), (y_nbr + far * (diag - y_nbr), (k + 2) % QUARTERS)

    def pass_on(k):
        (blk_x, q_x), (blk_y, q_y) = place(k)
        src_x, src_y = qref(blk_x, q_x), qref(blk_y, q_y)
        rcopy(src_x, src_x, row_send, recv_x.at[k], partner).wait_recv()
        rcopy(src_x, src_x, row_send, prime.at[k], partner).start()

        @pl.when(k < 2)
        def _():
            rcopy(src_x, src_x, row_send, recv_x.at[k + QUARTERS], y_nbr).start()

        rcopy(src_y, src_y, row_send, recv_y.at[k], partner).wait_recv()
        rcopy(src_y, src_y, row_send, prime.at[k], partner).start()

        @pl.when(k < 2)
        def _():
            rcopy(src_y, src_y, row_send, recv_y.at[k + QUARTERS], x_nbr).start()

    with jax.named_scope('pass_on'):
        pass_on(0)

    with jax.named_scope('aux_wait'):
        wait_aux(0, 2)
        start_aux(x_nbr, 2, partner)
        start_aux(y_nbr, 2, partner)
        start_aux(x_nbr, 3, y_nbr)

    with jax.named_scope('start_trips'):
        start_trips(place(0))

    @pl.loop(0, GROUPS)
    def _(k):
        pair = xbuf.at[0, pl.ds(0, 2 * quarter), :]
        with jax.named_scope('wait_prime'):
            rcopy(pair, pair, row_send, prime.at[k], partner).wait_recv()

        @pl.when(k == 0)
        def _():
            wait_aux(2, 2)

        @pl.when(k == QUARTERS - 1)
        def _():
            with jax.named_scope('energy'):
                pair_energy(x_nbr, y_nbr + ay * off_p)

        @pl.when(k == QUARTERS)
        def _():
            with jax.named_scope('share'):
                send_share()

        @pl.when(k < GROUPS - 1)
        def _():
            with jax.named_scope('pass_on'):
                pass_on(k + 1)

        @pl.when(k == QUARTERS - 1)
        def _():
            wait_aux(3)
            start_aux(diag, 4, partner)

        @pl.when(k == QUARTERS)
        def _():
            wait_aux(4)

        (blk_x, q_x), (blk_y, q_y) = place(k)
        with jax.named_scope('group'):
            trip([(blk_x, q_x), (blk_y, q_y), (blk_x + off_p, q_x), (blk_y + off_p, q_y)],
                 place(k + 1 - (k + 1) // GROUPS))

    sign = jnp.where(aux[me, 0:8, :] < 0.0, -1.0, 1.0)
    with jax.named_scope('force'):
        pull(last_p, last_it, upre[...])
        for grp in range(rows // 128):
            sl = slice(grp * 128, (grp + 1) * 128)
            row_sum = jnp.sum(sacc[:, sl], axis=0, keepdims=True)
            force = (row_sum * xti[0:width, sl].astype(F32) - tacc[:, sl]) * (sign[grp:grp + 1] * (1.0 / width))
            force_ref[sl, :] = jnp.transpose(force)

    with jax.named_scope('tail'):
        others = share_ref.at[pl.ds(0, 7)]
        rcopy(others, others, e_send, e_recv, partner).wait()
        rcopy(aux.at[pl.ds(0, 7)], aux.at[pl.ds(0, 7)], aux_send, aux_recv.at[0], partner).wait_send()
        rcopy(xbuf.at[pl.ds(0, 7)], xbuf.at[pl.ds(0, 7)], row_send, recv_p, partner).wait_send()


def finish(force_ref, share_ref, force_hbm, energy_hbm, energy, sem):
    rows = force_ref.shape[0]
    copies = []
    for n in range(4):
        sl = pl.ds(n * (rows // 4), rows // 4)
        copies.append(pltpu.make_async_copy(force_ref.at[sl, :], force_hbm.at[sl, :], sem.at[n]))
    copies.append(pltpu.make_async_copy(energy, energy_hbm, sem.at[4]))
    for cp in copies[:4]:
        cp.start()
    energy[0] = 0.5 * jnp.sum(jnp.sum(share_ref[...], axis=0))
    copies[4].start()
    for cp in copies:
        cp.wait()


def solution(mesh):
    def per_device(positions, charges, counts):
        rows, width = positions.shape
        dma = pltpu.SemaphoreType.DMA
        vmem, hbm = pl.BlockSpec(memory_space=pltpu.VMEM), pl.BlockSpec(memory_space=pltpu.HBM)
        force_type = jax.ShapeDtypeStruct((rows, width), F32)
        forces, shares = pl.pallas_call(
            kernel,
            out_shape=(force_type, jax.ShapeDtypeStruct((8, 8, 128), F32)),
            in_specs=[hbm, hbm, hbm],
            out_specs=(vmem, vmem),
            scratch_shapes=[
                pltpu.VMEM((8, rows, width), BF16),
                pltpu.VMEM((8, 16, 128), F32),
                pltpu.VMEM((2 * width, rows), BF16),
                pltpu.VMEM((2 * width, rows), BF16),
                pltpu.VMEM((8, rows), F32),
                pltpu.VMEM((8, 128), F32),
                pltpu.VMEM((rows // QUARTERS, TILE), F32),
                pltpu.VMEM((rows // QUARTERS, TILE), BF16),
                pltpu.VMEM((rows, 128), BF16),
                pltpu.VMEM((rows, 128), F32),
                pltpu.VMEM((8, rows), F32),
                pltpu.VMEM((width, rows), BF16),
                pltpu.VMEM((rows, 128), BF16),
                pltpu.VMEM((rows, 128), F32),
                pltpu.VMEM((8, rows), F32),
                pltpu.VMEM((width, rows), F32),
                pltpu.VMEM((8, 128), F32),
                pltpu.SMEM((1,), jnp.int32),
                dma((3,)), dma, dma, dma((5,)), dma, dma((GROUPS,)), dma((GROUPS,)), dma((GROUPS,)), dma, dma,
            ],
            compiler_params=pltpu.CompilerParams(collective_id=0, has_side_effects=True, vmem_limit_bytes=VMEM_LIMIT),
        )(counts, pltpu.with_memory_space_constraint(positions, pltpu.HBM),
          pltpu.with_memory_space_constraint(charges.reshape(8, 128), pltpu.HBM))
        return pl.pallas_call(
            finish,
            out_shape=(force_type, jax.ShapeDtypeStruct((1,), F32)),
            in_specs=[vmem, vmem],
            out_specs=(hbm, hbm),
            scratch_shapes=[pltpu.SMEM((1,), F32), dma((5,))],
            compiler_params=pltpu.CompilerParams(vmem_limit_bytes=4 * 1024 * 1024),
        )(forces, shares)

    row_spec = P(('sys', 'row'), None)
    vec_spec = P(('sys', 'row'))
    return jax.shard_map(per_device, mesh=mesh, in_specs=(row_spec, vec_spec, vec_spec), out_specs=(row_spec, P('sys')),
                         check_vma=False)
```

```python
import jax
import jax.numpy as jnp
from jax import lax
from jax.experimental import pallas as pl
from jax.experimental.pallas import tpu as pltpu
from jax.sharding import PartitionSpec as P

F32, BF16 = jnp.float32, jnp.bfloat16
LOG2E = 1.4426950408889634
NEG_BIG = -1e30
QUARTERS = 4
GROUPS = 6
TILE = 512
VMEM_LIMIT = 24 * 1024 * 1024


def split3(val):
    hi = val.astype(BF16).astype(F32)
    rest = val - hi
    mid = rest.astype(BF16).astype(F32)
    low = (rest - mid).astype(BF16).astype(F32)
    return hi, mid, low


def kernel(cnt_hbm, pos_hbm, q_hbm, sacc, tacc, xti, sign_ref, share_ref, xbuf, aux, xtp, pacc, ptot, gpre, upre, aug_e, cb_e, cap, xjt, aug, cb, qv, cnt,
           load_sem, row_send, aux_send, aux_recv, recv_p, recv_x, recv_y, prime, e_send, e_recv):
    rows, width = pos_hbm.shape
    quarter = rows // QUARTERS
    lanes_per = quarter // 128
    me = lax.axis_index('row')
    core, ax, ay = me % 2, (me // 2) % 2, me // 4
    off_p = 1 - 2 * core
    partner = me + off_p
    x_nbr = me + 2 - 4 * ax
    y_nbr = me + 4 - 8 * ay
    diag = x_nbr + 4 - 8 * ay

    def rcopy(src, dst, send, recv, dev):
        return pltpu.make_async_remote_copy(src_ref=src, dst_ref=dst, send_sem=send, recv_sem=recv,
                                            device_id={'row': dev}, device_id_type=pl.DeviceIdType.MESH)

    def qref(blk, q):
        return xbuf.at[blk, pl.ds(q * quarter, quarter), :]

    load = pltpu.make_async_copy(pos_hbm, xbuf.at[me], load_sem.at[0])
    load.start()
    load_q = pltpu.make_async_copy(q_hbm, qv, load_sem.at[1])
    load_q.start()
    load_c = pltpu.make_async_copy(cnt_hbm, cnt, load_sem.at[2])
    load_c.start()
    barrier = pltpu.get_barrier_semaphore()
    for dev in (partner, x_nbr, y_nbr):
        pl.semaphore_signal(barrier, inc=1, device_id={'row': dev}, device_id_type=pl.DeviceIdType.MESH)

    def send_quarter(k):
        rcopy(qref(me, k), qref(me, k), row_send, recv_x.at[k], x_nbr).start()
        qy = (k + 2) % QUARTERS
        rcopy(qref(me, qy), qref(me, qy), row_send, recv_y.at[k], y_nbr).start()

    load.wait()
    with jax.named_scope('bar_wait'):
        pl.semaphore_wait(barrier, 3)

    send_quarter(0)
    load_q.wait()
    load_c.wait()
    row_id = lax.broadcasted_iota(jnp.int32, (8, 128), 0) * 128 + lax.broadcasted_iota(jnp.int32, (8, 128), 1)
    live_q = jnp.where(row_id < cnt[0], qv[...], 0.0)
    aux[me, 0:8, :] = live_q

    def fill_lanes(dst, blk, log_q):
        half_sq = []
        for grp in range(rows // 128):
            sl = slice(grp * 128, (grp + 1) * 128)
            xt = jnp.transpose(xbuf[blk, sl, :])
            dst[0:width, sl] = xt
            if log_q is not None:
                xt = xt.astype(F32)
                half_sq.append(-0.5 * jnp.sum(xt * xt, axis=0, keepdims=True))
        if log_q is None:
            half_sq = aux[blk, 8:16, :]
        else:
            half_sq = jnp.concatenate(half_sq, axis=0)
            aux[blk, 8:16, :] = half_sq
        hi, mid, low = split3(half_sq if log_q is None else half_sq + log_q)
        sub16 = lax.broadcasted_iota(jnp.int32, (16, 128), 0)
        for grp in range(rows // 128):
            sl = slice(grp * 128, (grp + 1) * 128)
            row = slice(grp, grp + 1)
            piece = jnp.where(sub16 < 3, 1.0, jnp.where(sub16 == 3, hi[row], jnp.where(sub16 == 4, mid[row], jnp.where(
                sub16 == 5, low[row], 0.0))))
            dst[width:width + 16, sl] = piece.astype(BF16)

    abs_q = jnp.abs(live_q)
    log_q = jnp.where(abs_q > 0.0, jnp.log(jnp.where(abs_q > 0.0, abs_q, 1.0)) * float(width), NEG_BIG)
    fill_lanes(xti, me, log_q)
    for grp in range(rows // 128):
        cap[0:1, grp * 128:(grp + 1) * 128] = log_q[grp:grp + 1]
    for dst in (xti, xtp):
        dst[width + 16:2 * width, :] = jnp.zeros((width - 16, rows), BF16)
    for slot, dev in ((0, x_nbr), (0, y_nbr), (1, partner)):
        rcopy(aux.at[me], aux.at[me], aux_send, aux_recv.at[slot], dev).start()
    rcopy(xbuf.at[me], xbuf.at[me], row_send, recv_p, partner).start()
    for k in range(1, QUARTERS):
        send_quarter(k)
    sacc[...] = jnp.zeros_like(sacc)
    tacc[...] = jnp.zeros_like(tacc)

    def build(parts, first=0, cols=None, charges=None, pulls=True):
        cols, charges = aug if cols is None else cols, cb if charges is None else charges
        sub8 = lax.broadcasted_iota(jnp.int32, (8, 128), 0)
        for n, (blk, q) in enumerate(parts):
            for t in range(lanes_per):
                start = ((first + n) * lanes_per + t) * 128
                sl = slice(start, start + 128)
                grp = q * lanes_per + t
                if pulls:
                    xjt[:, sl] = jnp.transpose(xbuf[blk, pl.ds(pl.multiple_of(grp * 128, 128), 128), :])
                h, m, l = split3(aux[blk, pl.ds(8 + grp, 1), :])
                piece = jnp.where(sub8 == 0, h, jnp.where(sub8 == 1, m, jnp.where(sub8 == 2, l, jnp.where(
                    sub8 < 6, 1.0, 0.0))))
                piece = jnp.concatenate([piece, jnp.zeros((120, 128), F32)], axis=0)
                cols[sl, :] = jnp.transpose(piece).astype(BF16)
                charges[sl, :] = jnp.transpose(jnp.broadcast_to(aux[blk, pl.ds(grp, 1), :], (128, 128)))

    def gram(part, p, it, lanes=None, cols=None):
        lanes, cols = xti if lanes is None else lanes, aug if cols is None else cols
        blk, q = part
        xj = xbuf[blk, pl.ds(pl.multiple_of(q * quarter, quarter), quarter), :]
        lhs = jnp.concatenate([xj, cols[p * quarter:(p + 1) * quarter, :]], axis=1)
        return jnp.dot(lhs, lanes[:, it * TILE:(it + 1) * TILE], preferred_element_type=F32)

    tiles = rows // TILE
    units = [(p, it) for p in range(QUARTERS) for it in range(tiles)]
    last_p, last_it = units[-1]

    def pull(p, it, w_low):
        tacc[:, it * TILE:(it + 1) * TILE] += jnp.dot(xjt[:, p * quarter:(p + 1) * quarter], w_low,
                                                      preferred_element_type=F32)

    def weigh(p, it, product, own):
        sl = slice(it * TILE, (it + 1) * TILE)
        charge = jnp.concatenate([cb[p * quarter:(p + 1) * quarter, :]] * (TILE // 128), axis=1)
        weight = jnp.exp2(jnp.minimum(product, cap[0:1, sl]) * (LOG2E / width)) * charge
        if own and it * TILE <= p * quarter < (it + 1) * TILE:
            ri = lax.broadcasted_iota(jnp.int32, (quarter, TILE), 0) + (p * quarter - it * TILE)
            ci = lax.broadcasted_iota(jnp.int32, (quarter, TILE), 1)
            weight = jnp.where(ri == ci, 0.0, weight)
        ssum = sacc[:, sl]
        for t in range(quarter // 8):
            ssum = ssum + weight[t * 8:(t + 1) * 8, :]
        sacc[:, sl] = ssum
        return weight.astype(BF16)

    def compute(parts, own=False):
        build(parts)
        product = gram(parts[0], 0, 0)
        for idx, (p, it) in enumerate(units):
            w_low = weigh(p, it, product, own)
            if idx + 1 < len(units):
                n_p, n_it = units[idx + 1]
                product = gram(parts[n_p], n_p, n_it)
            pull(p, it, w_low)

    def start_trips(parts):
        build(parts)
        gpre[...] = gram(parts[0], 0, 0)
        upre[...] = jnp.zeros_like(upre)

    def trip(parts, next_parts):
        pull(last_p, last_it, upre[...])
        build(parts[2:], first=2)
        product = gpre[...]
        for idx, (p, it) in enumerate(units):
            w_low = weigh(p, it, product, False)
            if (p, it) == (1, tiles - 1):
                product = gram(parts[2], 2, 0)
                pull(p, it, w_low)
                build(next_parts)
            elif idx + 1 < len(units):
                n_p, n_it = units[idx + 1]
                product = gram(parts[n_p], n_p, n_it)
                pull(p, it, w_low)
            else:
                gpre[...] = gram(next_parts[0], 0, 0)
                upre[...] = w_low

    def pair_energy(row_blk, col_blk):
        fill_lanes(xtp, row_blk, None)
        parts = [(col_blk, q) for q in range(QUARTERS)]
        build(parts, cols=aug_e, charges=cb_e, pulls=False)
        for it in range(tiles):
            psum = jnp.zeros((8, TILE), F32)
            for p in range(QUARTERS):
                charge = jnp.concatenate([cb_e[p * quarter:(p + 1) * quarter, :]] * (TILE // 128), axis=1)
                product = gram(parts[p], p, it, lanes=xtp, cols=aug_e)
                weight = jnp.exp2(jnp.minimum(product, 0.0) * (LOG2E / width)) * charge
                for t in range(quarter // 8):
                    psum = psum + weight[t * 8:(t + 1) * 8, :]
            pacc[:, it * TILE:(it + 1) * TILE] = psum
        total = jnp.zeros((8, 128), F32)
        for grp in range(rows // 128):
            total = total + pacc[:, grp * 128:(grp + 1) * 128] * aux[row_blk, grp:grp + 1, :]
        ptot[...] = 2.0 * total

    def send_share():
        total = ptot[...]
        live_q = aux[me, 0:8, :]
        for grp in range(rows // 128):
            signed = jnp.where(live_q[grp:grp + 1] < 0.0, -1.0, 1.0) * sacc[:, grp * 128:(grp + 1) * 128]
            total = total + signed
        share_ref[me] = total
        for n in range(1, 8):
            rcopy(share_ref.at[me], share_ref.at[me], e_send, e_recv, (me + n) % 8).start()

    def wait_aux(slot, blocks=1):
        rcopy(aux.at[pl.ds(0, blocks)], aux.at[pl.ds(0, blocks)], aux_send, aux_recv.at[slot], partner).wait_recv()

    def start_aux(blk, slot, dev):
        rcopy(aux.at[blk], aux.at[blk], aux_send, aux_recv.at[slot], dev).start()

    with jax.named_scope('own'):
        compute([(me, q) for q in range(QUARTERS)], own=True)
    with jax.named_scope('partner_wait'):
        wait_aux(1)
        rcopy(xbuf.at[partner], xbuf.at[partner], row_send, recv_p, partner).wait_recv()
    with jax.named_scope('partner'):
        compute([(partner, q) for q in range(QUARTERS)])
    def place(k):
        far = k // QUARTERS
        return (x_nbr + far * (diag - x_nbr), k % QUARTERS), (y_nbr + far * (diag - y_nbr), (k + 2) % QUARTERS)

    def pass_on(k):
        (blk_x, q_x), (blk_y, q_y) = place(k)
        src_x, src_y = qref(blk_x, q_x), qref(blk_y, q_y)
        rcopy(src_x, src_x, row_send, recv_x.at[k], partner).wait_recv()
        rcopy(src_x, src_x, row_send, prime.at[k], partner).start()

        @pl.when(k < 2)
        def _():
            rcopy(src_x, src_x, row_send, recv_x.at[k + QUARTERS], y_nbr).start()

        rcopy(src_y, src_y, row_send, recv_y.at[k], partner).wait_recv()
        rcopy(src_y, src_y, row_send, prime.at[k], partner).start()

        @pl.when(k < 2)
        def _():
            rcopy(src_y, src_y, row_send, recv_y.at[k + QUARTERS], x_nbr).start()

    with jax.named_scope('pass_on'):
        pass_on(0)

    with jax.named_scope('aux_wait'):
        wait_aux(0, 2)
        start_aux(x_nbr, 2, partner)
        start_aux(y_nbr, 2, partner)
        start_aux(x_nbr, 3, y_nbr)

    with jax.named_scope('start_trips'):
        start_trips(place(0))

    @pl.loop(0, GROUPS)
    def _(k):
        pair = xbuf.at[0, pl.ds(0, 2 * quarter), :]
        with jax.named_scope('wait_prime'):
            rcopy(pair, pair, row_send, prime.at[k], partner).wait_recv()

        @pl.when(k == 0)
        def _():
            wait_aux(2, 2)

        @pl.when(k == QUARTERS - 1)
        def _():
            with jax.named_scope('energy'):
                pair_energy(x_nbr, y_nbr + ay * off_p)

        @pl.when(k == QUARTERS)
        def _():
            with jax.named_scope('share'):
                send_share()

        @pl.when(k < GROUPS - 1)
        def _():
            with jax.named_scope('pass_on'):
                pass_on(k + 1)

        @pl.when(k == QUARTERS - 1)
        def _():
            wait_aux(3)
            start_aux(diag, 4, partner)

        @pl.when(k == QUARTERS)
        def _():
            wait_aux(4)

        (blk_x, q_x), (blk_y, q_y) = place(k)
        with jax.named_scope('group'):
            trip([(blk_x, q_x), (blk_y, q_y), (blk_x + off_p, q_x), (blk_y + off_p, q_y)],
                 place(k + 1 - (k + 1) // GROUPS))

    sign_ref[...] = jnp.where(aux[me, 0:8, :] < 0.0, -1.0 / width, 1.0 / width)
    pull(last_p, last_it, upre[...])

    with jax.named_scope('tail'):
        others = share_ref.at[pl.ds(0, 7)]
        rcopy(others, others, e_send, e_recv, partner).wait()
        rcopy(aux.at[pl.ds(0, 7)], aux.at[pl.ds(0, 7)], aux_send, aux_recv.at[0], partner).wait_send()
        rcopy(xbuf.at[pl.ds(0, 7)], xbuf.at[pl.ds(0, 7)], row_send, recv_p, partner).wait_send()


def finish(sacc, tacc, xti, sign_ref, share_ref, force_hbm, energy_hbm, force, energy, sem):
    rows, width = force.shape
    copies = [pltpu.make_async_copy(energy, energy_hbm, sem.at[4])]
    for grp in range(rows // 128):
        sl = slice(grp * 128, (grp + 1) * 128)
        row_sum = jnp.sum(sacc[:, sl], axis=0, keepdims=True)
        value = (row_sum * xti[0:width, sl].astype(F32) - tacc[:, sl]) * sign_ref[grp:grp + 1]
        force[sl, :] = jnp.transpose(value)
        if grp % 2 == 1:
            part = pl.ds((grp - 1) * 128, 256)
            copies.append(pltpu.make_async_copy(force.at[part, :], force_hbm.at[part, :], sem.at[grp // 2]))
            copies[-1].start()
    energy[0] = 0.5 * jnp.sum(jnp.sum(share_ref[...], axis=0))
    copies[0].start()
    for cp in copies:
        cp.wait()


def solution(mesh):
    def per_device(positions, charges, counts):
        rows, width = positions.shape
        dma = pltpu.SemaphoreType.DMA
        vmem, hbm = pl.BlockSpec(memory_space=pltpu.VMEM), pl.BlockSpec(memory_space=pltpu.HBM)
        force_type = jax.ShapeDtypeStruct((rows, width), F32)
        parts = pl.pallas_call(
            kernel,
            out_shape=(jax.ShapeDtypeStruct((8, rows), F32), jax.ShapeDtypeStruct((width, rows), F32),
                       jax.ShapeDtypeStruct((2 * width, rows), BF16), jax.ShapeDtypeStruct((8, 128), F32),
                       jax.ShapeDtypeStruct((8, 8, 128), F32)),
            in_specs=[hbm, hbm, hbm],
            out_specs=(vmem,) * 5,
            scratch_shapes=[
                pltpu.VMEM((8, rows, width), BF16),
                pltpu.VMEM((8, 16, 128), F32),
                pltpu.VMEM((2 * width, rows), BF16),
                pltpu.VMEM((8, rows), F32),
                pltpu.VMEM((8, 128), F32),
                pltpu.VMEM((rows // QUARTERS, TILE), F32),
                pltpu.VMEM((rows // QUARTERS, TILE), BF16),
                pltpu.VMEM((rows, 128), BF16),
                pltpu.VMEM((rows, 128), F32),
                pltpu.VMEM((8, rows), F32),
                pltpu.VMEM((width, rows), BF16),
                pltpu.VMEM((rows, 128), BF16),
                pltpu.VMEM((rows, 128), F32),
                pltpu.VMEM((8, 128), F32),
                pltpu.SMEM((1,), jnp.int32),
                dma((3,)), dma, dma, dma((5,)), dma, dma((GROUPS,)), dma((GROUPS,)), dma((GROUPS,)), dma, dma,
            ],
            compiler_params=pltpu.CompilerParams(collective_id=0, has_side_effects=True, vmem_limit_bytes=VMEM_LIMIT),
        )(counts, pltpu.with_memory_space_constraint(positions, pltpu.HBM),
          pltpu.with_memory_space_constraint(charges.reshape(8, 128), pltpu.HBM))
        return pl.pallas_call(
            finish,
            out_shape=(force_type, jax.ShapeDtypeStruct((1,), F32)),
            in_specs=[vmem] * 5,
            out_specs=(hbm, hbm),
            scratch_shapes=[pltpu.VMEM((rows, width), F32), pltpu.SMEM((1,), F32), dma((5,))],
            compiler_params=pltpu.CompilerParams(vmem_limit_bytes=4 * 1024 * 1024),
        )(*parts)

    row_spec = P(('sys', 'row'), None)
    vec_spec = P(('sys', 'row'))
    return jax.shard_map(per_device, mesh=mesh, in_specs=(row_spec, vec_spec, vec_spec), out_specs=(row_spec, P('sys')),
                         check_vma=False)
```

```python
import jax
import jax.numpy as jnp
from jax import lax
from jax.experimental import pallas as pl
from jax.experimental.pallas import tpu as pltpu
from jax.sharding import PartitionSpec as P

F32, BF16 = jnp.float32, jnp.bfloat16
LOG2E = 1.4426950408889634
NEG_BIG = -1e30
QUARTERS = 4
GROUPS = 6
TILE = 256
LAG = 3
VMEM_LIMIT = 24 * 1024 * 1024


def split3(val):
    hi = val.astype(BF16).astype(F32)
    rest = val - hi
    mid = rest.astype(BF16).astype(F32)
    low = (rest - mid).astype(BF16).astype(F32)
    return hi, mid, low


def kernel(cnt_hbm, pos_hbm, q_hbm, force_ref, share_ref, xbuf, aux, xti, xtp, pacc, ptot, gpre, upre, aug_e, cb_e, cap, xjt, aug, cb, sacc, tacc, qv, cnt,
           load_sem, row_send, aux_send, aux_recv, recv_p, recv_x, recv_y, prime, e_send, e_recv):
    rows, width = pos_hbm.shape
    quarter = rows // QUARTERS
    lanes_per = quarter // 128
    me = lax.axis_index('row')
    core, ax, ay = me % 2, (me // 2) % 2, me // 4
    off_p = 1 - 2 * core
    partner = me + off_p
    x_nbr = me + 2 - 4 * ax
    y_nbr = me + 4 - 8 * ay
    diag = x_nbr + 4 - 8 * ay

    def rcopy(src, dst, send, recv, dev):
        return pltpu.make_async_remote_copy(src_ref=src, dst_ref=dst, send_sem=send, recv_sem=recv,
                                            device_id={'row': dev}, device_id_type=pl.DeviceIdType.MESH)

    def qref(blk, q):
        return xbuf.at[blk, pl.ds(q * quarter, quarter), :]

    load = pltpu.make_async_copy(pos_hbm, xbuf.at[me], load_sem.at[0])
    load.start()
    load_q = pltpu.make_async_copy(q_hbm, qv, load_sem.at[1])
    load_q.start()
    load_c = pltpu.make_async_copy(cnt_hbm, cnt, load_sem.at[2])
    load_c.start()
    barrier = pltpu.get_barrier_semaphore()
    for dev in (partner, x_nbr, y_nbr):
        pl.semaphore_signal(barrier, inc=1, device_id={'row': dev}, device_id_type=pl.DeviceIdType.MESH)

    def send_quarter(k):
        rcopy(qref(me, k), qref(me, k), row_send, recv_x.at[k], x_nbr).start()
        qy = (k + 2) % QUARTERS
        rcopy(qref(me, qy), qref(me, qy), row_send, recv_y.at[k], y_nbr).start()

    load_q.wait()
    load_c.wait()
    row_id = lax.broadcasted_iota(jnp.int32, (8, 128), 0) * 128 + lax.broadcasted_iota(jnp.int32, (8, 128), 1)
    live_q = jnp.where(row_id < cnt[0], qv[...], 0.0)
    aux[me, 0:8, :] = live_q
    load.wait()
    with jax.named_scope('bar_wait'):
        pl.semaphore_wait(barrier, 3)

    send_quarter(0)

    def fill_lanes(dst, blk, log_q):
        half_sq = []
        for grp in range(rows // 128):
            sl = slice(grp * 128, (grp + 1) * 128)
            xt = jnp.transpose(xbuf[blk, sl, :])
            dst[0:width, sl] = xt
            if log_q is not None:
                xt = xt.astype(F32)
                half_sq.append(-0.5 * jnp.sum(xt * xt, axis=0, keepdims=True))
        if log_q is None:
            half_sq = aux[blk, 8:16, :]
        else:
            half_sq = jnp.concatenate(half_sq, axis=0)
            aux[blk, 8:16, :] = half_sq
        hi, mid, low = split3(half_sq if log_q is None else half_sq + log_q)
        sub16 = lax.broadcasted_iota(jnp.int32, (16, 128), 0)
        for grp in range(rows // 128):
            sl = slice(grp * 128, (grp + 1) * 128)
            row = slice(grp, grp + 1)
            piece = jnp.where(sub16 < 3, 1.0, jnp.where(sub16 == 3, hi[row], jnp.where(sub16 == 4, mid[row], jnp.where(
                sub16 == 5, low[row], 0.0))))
            dst[width:width + 16, sl] = piece.astype(BF16)

    abs_q = jnp.abs(live_q)
    log_q = jnp.where(abs_q > 0.0, jnp.log(jnp.where(abs_q > 0.0, abs_q, 1.0)) * float(width), NEG_BIG)
    fill_lanes(xti, me, log_q)
    for grp in range(rows // 128):
        cap[0:1, grp * 128:(grp + 1) * 128] = log_q[grp:grp + 1]
    for dst in (xti, xtp):
        dst[width + 16:2 * width, :] = jnp.zeros((width - 16, rows), BF16)
    for slot, dev in ((0, x_nbr), (0, y_nbr), (1, partner)):
        rcopy(aux.at[me], aux.at[me], aux_send, aux_recv.at[slot], dev).start()
    rcopy(xbuf.at[me], xbuf.at[me], row_send, recv_p, partner).start()
    for k in range(1, QUARTERS):
        send_quarter(k)
    sacc[...] = jnp.zeros_like(sacc)
    tacc[...] = jnp.zeros_like(tacc)

    def build(parts, first=0, cols=None, charges=None, pulls=True):
        cols, charges = aug if cols is None else cols, cb if charges is None else charges
        sub8 = lax.broadcasted_iota(jnp.int32, (8, 128), 0)
        for n, (blk, q) in enumerate(parts):
            for t in range(lanes_per):
                start = ((first + n) * lanes_per + t) * 128
                sl = slice(start, start + 128)
                grp = q * lanes_per + t
                if pulls:
                    xjt[:, sl] = jnp.transpose(xbuf[blk, pl.ds(pl.multiple_of(grp * 128, 128), 128), :])
                h, m, l = split3(aux[blk, pl.ds(8 + grp, 1), :])
                piece = jnp.where(sub8 == 0, h, jnp.where(sub8 == 1, m, jnp.where(sub8 == 2, l, jnp.where(
                    sub8 < 6, 1.0, 0.0))))
                piece = jnp.concatenate([piece, jnp.zeros((120, 128), F32)], axis=0)
                cols[sl, :] = jnp.transpose(piece).astype(BF16)
                charges[sl, :] = jnp.transpose(jnp.broadcast_to(aux[blk, pl.ds(grp, 1), :], (128, 128)))

    def gram(part, p, it, lanes=None, cols=None):
        lanes, cols = xti if lanes is None else lanes, aug if cols is None else cols
        blk, q = part
        xj = xbuf[blk, pl.ds(pl.multiple_of(q * quarter, quarter), quarter), :]
        lhs = jnp.concatenate([xj, cols[p * quarter:(p + 1) * quarter, :]], axis=1)
        return jnp.dot(lhs, lanes[:, it * TILE:(it + 1) * TILE], preferred_element_type=F32)

    tiles = rows // TILE
    units = [(p, it) for p in range(QUARTERS) for it in range(tiles)]
    last_p, last_it = units[-1]

    def pull(p, it, w_low):
        tacc[:, it * TILE:(it + 1) * TILE] += jnp.dot(xjt[:, p * quarter:(p + 1) * quarter], w_low,
                                                      preferred_element_type=F32)

    def weigh(p, it, product, own):
        sl = slice(it * TILE, (it + 1) * TILE)
        charge = jnp.concatenate([cb[p * quarter:(p + 1) * quarter, :]] * (TILE // 128), axis=1)
        weight = jnp.exp2(jnp.minimum(product, cap[0:1, sl]) * (LOG2E / width)) * charge
        if own and it * TILE <= p * quarter < (it + 1) * TILE:
            ri = lax.broadcasted_iota(jnp.int32, (quarter, TILE), 0) + (p * quarter - it * TILE)
            ci = lax.broadcasted_iota(jnp.int32, (quarter, TILE), 1)
            weight = jnp.where(ri == ci, 0.0, weight)
        ssum = sacc[:, sl]
        for t in range(quarter // 8):
            ssum = ssum + weight[t * 8:(t + 1) * 8, :]
        sacc[:, sl] = ssum
        return weight.astype(BF16)

    def compute(parts, own=False):
        build(parts)
        products = [gram(parts[p], p, it) for p, it in units[:LAG]]
        for idx, (p, it) in enumerate(units):
            w_low = weigh(p, it, products.pop(0), own)
            if idx + LAG < len(units):
                n_p, n_it = units[idx + LAG]
                products.append(gram(parts[n_p], n_p, n_it))
            pull(p, it, w_low)

    def start_trips(parts):
        build(parts)
        for n, (p, it) in enumerate(units[:LAG]):
            gpre[n] = gram(parts[p], p, it)
        upre[...] = jnp.zeros_like(upre)

    def trip(parts, next_parts):
        pull(last_p, last_it, upre[...])
        build(parts[2:], first=2)
        products = [gpre[n] for n in range(LAG)]
        for idx, (p, it) in enumerate(units):
            w_low = weigh(p, it, products.pop(0), False)
            if idx + LAG < len(units):
                n_p, n_it = units[idx + LAG]
                products.append(gram(parts[n_p], n_p, n_it))
            else:
                n = idx + LAG - len(units)
                n_p, n_it = units[n]
                gpre[n] = gram(next_parts[n_p], n_p, n_it)
            if idx + 1 < len(units):
                pull(p, it, w_low)
            else:
                upre[...] = w_low
            if (p, it) == (1, tiles - 1):
                build(next_parts)

    def pair_energy(row_blk, col_blk):
        fill_lanes(xtp, row_blk, None)
        parts = [(col_blk, q) for q in range(QUARTERS)]
        build(parts, cols=aug_e, charges=cb_e, pulls=False)
        for it in range(tiles):
            psum = jnp.zeros((8, TILE), F32)
            for p in range(QUARTERS):
                charge = jnp.concatenate([cb_e[p * quarter:(p + 1) * quarter, :]] * (TILE // 128), axis=1)
                product = gram(parts[p], p, it, lanes=xtp, cols=aug_e)
                weight = jnp.exp2(jnp.minimum(product, 0.0) * (LOG2E / width)) * charge
                for t in range(quarter // 8):
                    psum = psum + weight[t * 8:(t + 1) * 8, :]
            pacc[:, it * TILE:(it + 1) * TILE] = psum
        total = jnp.zeros((8, 128), F32)
        for grp in range(rows // 128):
            total = total + pacc[:, grp * 128:(grp + 1) * 128] * aux[row_blk, grp:grp + 1, :]
        ptot[...] = 2.0 * total

    def send_share():
        total = ptot[...]
        live_q = aux[me, 0:8, :]
        for grp in range(rows // 128):
            signed = jnp.where(live_q[grp:grp + 1] < 0.0, -1.0, 1.0) * sacc[:, grp * 128:(grp + 1) * 128]
            total = total + signed
        share_ref[me] = total
        for n in range(1, 8):
            rcopy(share_ref.at[me], share_ref.at[me], e_send, e_recv, (me + n) % 8).start()

    def wait_aux(slot, blocks=1):
        rcopy(aux.at[pl.ds(0, blocks)], aux.at[pl.ds(0, blocks)], aux_send, aux_recv.at[slot], partner).wait_recv()

    def start_aux(blk, slot, dev):
        rcopy(aux.at[blk], aux.at[blk], aux_send, aux_recv.at[slot], dev).start()

    with jax.named_scope('own'):
        compute([(me, q) for q in range(QUARTERS)], own=True)
    with jax.named_scope('partner_wait'):
        wait_aux(1)
        rcopy(xbuf.at[partner], xbuf.at[partner], row_send, recv_p, partner).wait_recv()
    with jax.named_scope('partner'):
        compute([(partner, q) for q in range(QUARTERS)])
    def place(k):
        far = k // QUARTERS
        return (x_nbr + far * (diag - x_nbr), k % QUARTERS), (y_nbr + far * (diag - y_nbr), (k + 2) % QUARTERS)

    def pass_on(k):
        (blk_x, q_x), (blk_y, q_y) = place(k)
        src_x, src_y = qref(blk_x, q_x), qref(blk_y, q_y)
        rcopy(src_x, src_x, row_send, recv_x.at[k], partner).wait_recv()
        rcopy(src_x, src_x, row_send, prime.at[k], partner).start()

        @pl.when(k < 2)
        def _():
            rcopy(src_x, src_x, row_send, recv_x.at[k + QUARTERS], y_nbr).start()

        rcopy(src_y, src_y, row_send, recv_y.at[k], partner).wait_recv()
        rcopy(src_y, src_y, row_send, prime.at[k], partner).start()

        @pl.when(k < 2)
        def _():
            rcopy(src_y, src_y, row_send, recv_y.at[k + QUARTERS], x_nbr).start()

    with jax.named_scope('pass_on'):
        pass_on(0)

    with jax.named_scope('aux_wait'):
        wait_aux(0, 2)
        start_aux(x_nbr, 2, partner)
        start_aux(y_nbr, 2, partner)
        start_aux(x_nbr, 3, y_nbr)

    with jax.named_scope('start_trips'):
        start_trips(place(0))

    @pl.loop(0, GROUPS)
    def _(k):
        pair = xbuf.at[0, pl.ds(0, 2 * quarter), :]
        with jax.named_scope('wait_prime'):
            rcopy(pair, pair, row_send, prime.at[k], partner).wait_recv()

        @pl.when(k == 0)
        def _():
            wait_aux(2, 2)

        @pl.when(k == QUARTERS - 1)
        def _():
            with jax.named_scope('energy'):
                pair_energy(x_nbr, y_nbr + ay * off_p)

        @pl.when(k == QUARTERS)
        def _():
            with jax.named_scope('share'):
                send_share()

        @pl.when(k < GROUPS - 1)
        def _():
            with jax.named_scope('pass_on'):
                pass_on(k + 1)

        @pl.when(k == QUARTERS - 1)
        def _():
            wait_aux(3)
            start_aux(diag, 4, partner)

        @pl.when(k == QUARTERS)
        def _():
            wait_aux(4)

        (blk_x, q_x), (blk_y, q_y) = place(k)
        with jax.named_scope('group'):
            trip([(blk_x, q_x), (blk_y, q_y), (blk_x + off_p, q_x), (blk_y + off_p, q_y)],
                 place(k + 1 - (k + 1) // GROUPS))

    sign = jnp.where(aux[me, 0:8, :] < 0.0, -1.0, 1.0)
    with jax.named_scope('force'):
        pull(last_p, last_it, upre[...])
        for grp in range(rows // 128):
            sl = slice(grp * 128, (grp + 1) * 128)
            row_sum = jnp.sum(sacc[:, sl], axis=0, keepdims=True)
            force = (row_sum * xti[0:width, sl].astype(F32) - tacc[:, sl]) * (sign[grp:grp + 1] * (1.0 / width))
            force_ref[sl, :] = jnp.transpose(force)

    with jax.named_scope('tail'):
        others = share_ref.at[pl.ds(0, 7)]
        rcopy(others, others, e_send, e_recv, partner).wait()
        rcopy(aux.at[pl.ds(0, 7)], aux.at[pl.ds(0, 7)], aux_send, aux_recv.at[0], partner).wait_send()
        rcopy(xbuf.at[pl.ds(0, 7)], xbuf.at[pl.ds(0, 7)], row_send, recv_p, partner).wait_send()


def finish(force_ref, share_ref, force_hbm, energy_hbm, energy, sem):
    rows = force_ref.shape[0]
    copies = []
    for n in range(4):
        sl = pl.ds(n * (rows // 4), rows // 4)
        copies.append(pltpu.make_async_copy(force_ref.at[sl, :], force_hbm.at[sl, :], sem.at[n]))
    copies.append(pltpu.make_async_copy(energy, energy_hbm, sem.at[4]))
    for cp in copies[:4]:
        cp.start()
    energy[0] = 0.5 * jnp.sum(jnp.sum(share_ref[...], axis=0))
    copies[4].start()
    for cp in copies:
        cp.wait()


def solution(mesh):
    def per_device(positions, charges, counts):
        rows, width = positions.shape
        dma = pltpu.SemaphoreType.DMA
        vmem, hbm = pl.BlockSpec(memory_space=pltpu.VMEM), pl.BlockSpec(memory_space=pltpu.HBM)
        force_type = jax.ShapeDtypeStruct((rows, width), F32)
        forces, shares = pl.pallas_call(
            kernel,
            out_shape=(force_type, jax.ShapeDtypeStruct((8, 8, 128), F32)),
            in_specs=[hbm, hbm, hbm],
            out_specs=(vmem, vmem),
            scratch_shapes=[
                pltpu.VMEM((8, rows, width), BF16),
                pltpu.VMEM((8, 16, 128), F32),
                pltpu.VMEM((2 * width, rows), BF16),
                pltpu.VMEM((2 * width, rows), BF16),
                pltpu.VMEM((8, rows), F32),
                pltpu.VMEM((8, 128), F32),
                pltpu.VMEM((LAG, rows // QUARTERS, TILE), F32),
                pltpu.VMEM((rows // QUARTERS, TILE), BF16),
                pltpu.VMEM((rows, 128), BF16),
                pltpu.VMEM((rows, 128), F32),
                pltpu.VMEM((8, rows), F32),
                pltpu.VMEM((width, rows), BF16),
                pltpu.VMEM((rows, 128), BF16),
                pltpu.VMEM((rows, 128), F32),
                pltpu.VMEM((8, rows), F32),
                pltpu.VMEM((width, rows), F32),
                pltpu.VMEM((8, 128), F32),
                pltpu.SMEM((1,), jnp.int32),
                dma((3,)), dma, dma, dma((5,)), dma, dma((GROUPS,)), dma((GROUPS,)), dma((GROUPS,)), dma, dma,
            ],
            compiler_params=pltpu.CompilerParams(collective_id=0, has_side_effects=True, vmem_limit_bytes=VMEM_LIMIT),
        )(counts, pltpu.with_memory_space_constraint(positions, pltpu.HBM),
          pltpu.with_memory_space_constraint(charges.reshape(8, 128), pltpu.HBM))
        return pl.pallas_call(
            finish,
            out_shape=(force_type, jax.ShapeDtypeStruct((1,), F32)),
            in_specs=[vmem, vmem],
            out_specs=(hbm, hbm),
            scratch_shapes=[pltpu.SMEM((1,), F32), dma((5,))],
            compiler_params=pltpu.CompilerParams(vmem_limit_bytes=4 * 1024 * 1024),
        )(forces, shares)

    row_spec = P(('sys', 'row'), None)
    vec_spec = P(('sys', 'row'))
    return jax.shard_map(per_device, mesh=mesh, in_specs=(row_spec, vec_spec, vec_spec), out_specs=(row_spec, P('sys')),
                         check_vma=False)
```
